256 devices in a mesh: dp: 8 (over y, x_hi), tok: 16 (over z, core), col: 2 (over x_lo).
Axes of the slice: x: 4 (x_hi: 2, x_lo: 2; x = x_hi * 2 + x_lo), y: 4, z: 8, core: 2. Of those that a mesh axis runs over, the one named last changes fastest.
Arguments:
- tokens: bfloat16 [8, 8192, 1024], P('dp', 'tok'), may hold values from -6 to 6
- ln_gain: bfloat16 [1024], replicated, may hold values from 0.099609375 to 1.8984375
- qkv_weight: bfloat16 [3, 1024, 512], P(None, None, 'col'), may hold values from -0.375 to 0.375
- out_weight: bfloat16 [512, 1024], P('col'), may hold values from -0.25 to 0.25
- readout_weight: bfloat16 [1024, 64], replicated, may hold values from -0.1875 to 0.1875
- conv_weight: bfloat16 [2, 64, 576], replicated, may hold values from -0.25 to 0.25
- head_weight: bfloat16 [2, 64], replicated, may hold values from -0.75 to 0.75
- holo_cot: float32 [8, 2, 32, 256], P('dp', None, 'tok', 'col'), may hold values from -1 to 1
Outputs:
- hologram: float32 [8, 2, 32, 256], P('dp', None, 'tok', 'col')
- conv_grad: float32 [2, 64, 576], replicated
- out_grad: float32 [512, 1024], P('col')
The draws below stay inside these ranges and needn't reach their ends.
All inputs are finite; a program needn't handle non-finite values.
Results may differ from the reference program's by a relative error of at most 0.017.
The reference program's roundings to bfloat16 on the way count: a program that leaves them out, or rounds other values in their place, can miss the bound.
Values may be sent and summed in bfloat16 or wider, within the bound.
A program may use at most 128 MiB of HBM per device.

```python
import jax
import jax.numpy as jnp
from jax import lax

D = 1024
HEAD = 64
HEADS = 8
CH = 64
COLS = 256
LAYERS = 2
LENGTH = 8192
FRAMES = 8
ROWS = 32
HW = 512


def draw_tokens(key, part):
    noise = jax.random.normal(jax.random.fold_in(key, 11), (FRAMES, LENGTH, D), jnp.float32)
    return jnp.clip(noise, -6.0, 6.0).astype(jnp.bfloat16)


def draw_qkv_weight(key, part):
    factors = jnp.array([2.0, 2.0, 1.0], jnp.float32).reshape(3, 1, 1)
    drawn = jax.random.normal(jax.random.fold_in(key, 21), (3, D, HW), jnp.float32) * factors / jnp.sqrt(D * 1.0)
    bound = 12.0 / jnp.sqrt(D * 1.0)
    return jnp.clip(drawn, -bound, bound).astype(jnp.bfloat16)


def block_scale(stream_key, extent, cuts, least, largest):
    gain = 1.0
    for axis_at, blocks in cuts:
        heights = jax.random.uniform(jax.random.fold_in(jax.random.fold_in(stream_key, 6), axis_at), (blocks,), jnp.float32, least / len(cuts), largest / len(cuts))
        gain = gain * jnp.repeat(jnp.exp(heights), extent[axis_at] // blocks).reshape((-1,) + (1,) * (len(extent) - 1 - axis_at))
    return gain


def bell_draw(key, shape, scale, reach, cuts=(), kind=jnp.bfloat16):
    entries = jax.random.normal(key, shape, jnp.float32) * scale
    if len(cuts) > 0:
        entries = block_scale(key, shape, cuts, -0.22, 0.18) * entries
    return jnp.clip(entries, min=-reach, max=reach).astype(kind)


def setup_inputs(seed: int = 0) -> dict:
    arg_keys = jax.random.split(jax.random.key(seed), 9)
    return {
        "tokens": draw_tokens(jax.random.fold_in(arg_keys[8], 71), 0),
        "ln_gain": jnp.clip(1.0 + 0.18 * jax.random.normal(arg_keys[1], (D,), jnp.float32), 0.099609375, 1.8984375).astype(jnp.bfloat16),
        "qkv_weight": draw_qkv_weight(jax.random.fold_in(arg_keys[8], 71), 0),
        "out_weight": bell_draw(arg_keys[3], (HW, D), HW ** -0.5, 0.25, ((0, 2),)),
        "readout_weight": bell_draw(arg_keys[4], (D, CH), D ** -0.5, 0.1875),
        "conv_weight": bell_draw(arg_keys[5], (LAYERS, CH, 9 * CH), (9 * CH) ** -0.5, 0.25),
        "head_weight": bell_draw(arg_keys[6], (2, CH), CH ** -0.5, 0.75),
        "holo_cot": bell_draw(arg_keys[7], (FRAMES, 2, ROWS, COLS), (16.0 / (FRAMES * LENGTH) ** 0.5), 1.0, ((0, 8), (2, 16), (3, 2)), jnp.float32),
    }


EPSILON = 1e-05

def normalize(rows_in, ln_gain):
    values = rows_in.astype(jnp.float32)
    center = values - lax.optimization_barrier(jnp.mean(values, axis=-1, keepdims=True))
    spread = lax.optimization_barrier(jnp.mean(center * center, axis=-1, keepdims=True))
    return (center * lax.rsqrt(spread + EPSILON) * ln_gain.astype(jnp.float32)).astype(jnp.bfloat16)

def attend(queries, key_rows, value_rows):
    length = queries.shape[0]
    block_rows = min(512, length)
    query_blocks = queries.reshape(length // block_rows, block_rows, HEADS, HEAD)
    key_view = key_rows.reshape(length, HEADS, HEAD).astype(jnp.float32)
    value_view = value_rows.reshape(length, HEADS, HEAD)

    def one_block(query_block):
        scores = jnp.einsum('qhd,khd->hqk', query_block.astype(jnp.float32), key_view) * (1.0 / HEAD ** 0.5)
        row_top = lax.optimization_barrier(jnp.max(scores, axis=-1, keepdims=True))
        raised = jnp.exp(scores - row_top)
        row_total = lax.optimization_barrier(jnp.sum(raised, axis=-1))
        weights = raised.astype(jnp.bfloat16)
        weighted = jnp.einsum('hqk,khd->qhd', weights.astype(jnp.float32), value_view.astype(jnp.float32))
        return (weighted / jnp.transpose(row_total)[:, :, None]).astype(jnp.bfloat16)
    context = lax.map(one_block, query_blocks)
    return context.reshape(length, HEADS * HEAD)

def neighbourhood(padded, grid_rows, grid_cols):
    pieces = [padded[:, row_off:row_off + grid_rows, col_off:col_off + grid_cols] for row_off in range(3) for col_off in range(3)]
    return jnp.concatenate(pieces, axis=0).reshape(9 * padded.shape[0], grid_rows * grid_cols)

def flipped(padded, grid_rows, grid_cols):
    pieces = [padded[:, 2 - row_off:2 - row_off + grid_rows, 2 - col_off:2 - col_off + grid_cols] for row_off in range(3) for col_off in range(3)]
    return jnp.concatenate(pieces, axis=0).reshape(9 * padded.shape[0], grid_rows * grid_cols)

def transposed(weight):
    channels = weight.shape[0]
    return jnp.transpose(weight.reshape(channels, 9, channels), (2, 1, 0)).reshape(channels, 9 * channels)

def frame_network(first_map, conv_weight, head_weight, cotangent):
    channels, grid_rows, grid_cols = first_map.shape
    hidden = first_map
    inputs = []
    pre_acts = []
    for layer_at in range(LAYERS):
        padded = jnp.pad(hidden, ((0, 0), (1, 1), (1, 1)))
        stacked = neighbourhood(padded, grid_rows, grid_cols)
        pre_act = jnp.dot(conv_weight[layer_at], stacked, preferred_element_type=jnp.float32)
        inputs.append(stacked)
        pre_acts.append(pre_act)
        hidden = jax.nn.silu(pre_act).astype(jnp.bfloat16).reshape(channels, grid_rows, grid_cols)
    hologram = jnp.dot(head_weight, hidden.reshape(channels, -1), preferred_element_type=jnp.float32)
    grad_hidden = jnp.dot(jnp.transpose(head_weight.astype(jnp.float32)), cotangent.reshape(cotangent.shape[0], -1), precision=lax.Precision.HIGHEST).astype(jnp.bfloat16)
    conv_terms = [None] * LAYERS
    for layer_at in reversed(range(LAYERS)):
        pre_act = pre_acts[layer_at]
        sigmoid_pre = jax.nn.sigmoid(pre_act)
        grad_pre = (grad_hidden.reshape(channels, -1).astype(jnp.float32) * sigmoid_pre * (1.0 + pre_act * (1.0 - sigmoid_pre))).astype(jnp.bfloat16)
        conv_terms[layer_at] = lax.dot_general(grad_pre, inputs[layer_at], (((1,), (1,)), ((), ())), preferred_element_type=jnp.float32)
        padded = jnp.pad(grad_pre.reshape(channels, grid_rows, grid_cols), ((0, 0), (1, 1), (1, 1)))
        grad_hidden = jnp.dot(transposed(conv_weight[layer_at]), flipped(padded, grid_rows, grid_cols), preferred_element_type=jnp.float32).astype(jnp.bfloat16)
    return (hologram.reshape(cotangent.shape), jnp.stack(conv_terms), grad_hidden)

def reference(tokens, ln_gain, qkv_weight, out_weight, readout_weight, conv_weight, head_weight, holo_cot):

    def one_frame(inputs_pair):
        rows_in, cotangent = inputs_pair
        normed = normalize(rows_in, ln_gain)
        queries = jnp.dot(normed, qkv_weight[0], preferred_element_type=jnp.float32).astype(jnp.bfloat16)
        key_rows = jnp.dot(normed, qkv_weight[1], preferred_element_type=jnp.float32).astype(jnp.bfloat16)
        value_rows = jnp.dot(normed, qkv_weight[2], preferred_element_type=jnp.float32).astype(jnp.bfloat16)
        context = attend(queries, key_rows, value_rows)
        mixed = rows_in.astype(jnp.float32) + jnp.dot(context, out_weight, preferred_element_type=jnp.float32)
        readout = jnp.dot(mixed, readout_weight.astype(jnp.float32), precision=lax.Precision.HIGHEST).astype(jnp.bfloat16)
        first_map = jnp.transpose(readout).reshape(CH, ROWS, COLS)
        hologram, conv_terms, grad_readout = frame_network(first_map, conv_weight, head_weight, cotangent)
        small_term = lax.dot_general(context, grad_readout, (((0,), (1,)), ((), ())), preferred_element_type=jnp.float32)
        return (hologram, conv_terms, small_term)
    holograms, conv_all, small_all = lax.map(one_frame, (tokens, holo_cot))
    grad_small = lax.optimization_barrier(jnp.sum(small_all, axis=0))
    out_grad = jnp.dot(grad_small, jnp.transpose(readout_weight.astype(jnp.float32)), precision=lax.Precision.HIGHEST)
    return (holograms, lax.optimization_barrier(jnp.sum(conv_all, axis=0)), out_grad)
```

```python
import functools

import jax
import jax.numpy as jnp
from jax import lax
from jax.experimental import pallas as pl
from jax.experimental.pallas import tpu as pltpu
from jax.sharding import PartitionSpec as P

HEAD = 64
EPSILON = 1e-05
MESH = pl.DeviceIdType.MESH
F32 = jnp.float32
BF16 = jnp.bfloat16

NT = (((1,), (1,)), ((), ()))


def dot_nt(a, b):
    return lax.dot_general(a, b, NT, preferred_element_type=F32)


def dot_nn(a, b):
    return jnp.dot(a, b, preferred_element_type=F32)


def remote(src, dst, send_sem, recv_sem, where):
    return pltpu.make_async_remote_copy(
        src_ref=src,
        dst_ref=dst,
        send_sem=send_sem,
        recv_sem=recv_sem,
        device_id=where,
        device_id_type=MESH,
    )


QT = 256
LN_ROWS = 128


def attend_block(zs, qz, kvb, vx, m_ref, acc_ref):
    rows = kvb.shape[2]
    lane = lax.broadcasted_iota(jnp.int32, (rows, 128), 1)
    for half in range(2):
        for pair in range(2):
            v = kvb[2 * zs + half, 1, :, 128 * pair : 128 * pair + 128]
            one = jnp.ones_like(v)
            vx[2 * pair, half * rows : (half + 1) * rows, :] = jnp.where(lane < HEAD, v, one)
            vx[2 * pair + 1, half * rows : (half + 1) * rows, :] = jnp.where(lane < HEAD, one, v)

    def tile(qt, carry):
        at = pl.ds(pl.multiple_of(qt * QT, QT), QT)
        for h in range(4):
            pair = h // 2
            q = qz[h, at, :]
            s = [
                dot_nt(q, kvb[2 * zs + half, 0, :, 128 * pair : 128 * pair + 128])
                for half in range(2)
            ]
            m_old = m_ref[h, at, :]
            top = jnp.maximum(
                jnp.max(s[0], axis=1, keepdims=True), jnp.max(s[1], axis=1, keepdims=True)
            )
            m_new = jnp.maximum(m_old, top)
            wide = jnp.concatenate([m_new] * (rows // 128), axis=1)
            out = None
            for half in range(2):
                p = jnp.exp(s[half] - wide).astype(BF16)
                o = dot_nn(p, vx[h, half * rows : (half + 1) * rows, :])
                out = o if out is None else out + o
            acc_ref[h, at, :] = acc_ref[h, at, :] * jnp.exp(m_old - m_new) + out
            m_ref[h, at, :] = m_new
        return carry

    lax.fori_loop(0, qz.shape[1] // QT, tile, 0)


def attention_kernel(
    tok_ref, gain_ref, w_ref, ctx_ref, qz, kvb, vx, m_ref, acc_ref, send_sem, recv_sem
):
    t = lax.axis_index("tok")
    n_z = lax.axis_size("tok") // 2
    z, c = t // 2, lax.rem(t, 2)
    up = lax.rem(z + 1, n_z) * 2 + c
    down = lax.rem(z + n_z - 1, n_z) * 2 + c
    mate = z * 2 + 1 - c

    barrier = pltpu.get_barrier_semaphore()
    for peer in (up, down, mate):
        pl.semaphore_signal(barrier, inc=1, device_id={"tok": peer}, device_id_type=MESH)

    rows_all, width = tok_ref.shape

    def project(r, carry):
        at = pl.ds(pl.multiple_of(r * LN_ROWS, LN_ROWS), LN_ROWS)
        x = tok_ref[at, :].astype(F32)
        center = x - jnp.mean(x, axis=-1, keepdims=True)
        spread = jnp.mean(center * center, axis=-1, keepdims=True)
        normed = (center * lax.rsqrt(spread + EPSILON) * gain_ref[...].astype(F32)).astype(BF16)
        q = (dot_nn(normed, w_ref[0]).astype(BF16).astype(F32) * (1.0 / HEAD**0.5)).astype(BF16)
        kvb[t, 0, at, :] = dot_nn(normed, w_ref[1]).astype(BF16)
        kvb[t, 1, at, :] = dot_nn(normed, w_ref[2]).astype(BF16)
        lane = lax.broadcasted_iota(jnp.int32, (LN_ROWS, 128), 1)
        for pair in range(2):
            part = q[:, 128 * pair : 128 * pair + 128]
            none = jnp.zeros_like(part)
            qz[2 * pair, at, :] = jnp.where(lane < HEAD, part, none)
            qz[2 * pair + 1, at, :] = jnp.where(lane < HEAD, none, part)
        return carry

    lax.fori_loop(0, rows_all // LN_ROWS, project, 0)
    m_ref[...] = jnp.full(m_ref.shape, -1e30, F32)
    acc_ref[...] = jnp.zeros(acc_ref.shape, F32)
    pl.semaphore_wait(barrier, 3)

    def copy(blk, kv, lane_of, peer):
        piece = kvb.at[blk, kv]
        return remote(
            piece, piece, send_sem.at[lane_of, blk, kv], recv_sem.at[blk, kv], {"tok": peer}
        )

    for kv in range(2):
        copy(t, kv, 0, up).start()
        copy(t, kv, 1, down).start()
        copy(t, kv, 2, mate).start()

    def blocks(d):
        low = lax.rem(z - d + n_z, n_z)
        high = lax.rem(z + d, n_z)
        return low, high

    def turn(d, carry):
        low, high = blocks(d)

        @pl.when(jnp.logical_and(d >= 1, d <= 3))
        def _():
            for kv in range(2):
                b_low, b_high = low * 2 + c, high * 2 + c
                copy(b_low, kv, 0, up).wait_recv()

                @pl.when(d <= (3 if kv == 0 else 2))
                def _():
                    copy(b_low, kv, 0, up).start()

                copy(b_low, kv, 2, mate).start()
                copy(b_high, kv, 1, down).wait_recv()

                @pl.when(d <= (3 if kv == 1 else 2))
                def _():
                    copy(b_high, kv, 1, down).start()

                copy(b_high, kv, 2, mate).start()

        @pl.when(d == 4)
        def _():
            for kv in range(2):
                copy(low * 2 + c, kv, 0, up).wait_recv()
                copy(low * 2 + c, kv, 2, mate).start()

        for kv in range(2):
            copy(low * 2 + 1 - c, kv, 2, mate).wait_recv()

        @pl.when(jnp.logical_and(d >= 1, d <= 3))
        def _():
            for kv in range(2):
                copy(high * 2 + 1 - c, kv, 2, mate).wait_recv()

        def one(j, inner):
            attend_block(low * (1 - j) + high * j, qz, kvb, vx, m_ref, acc_ref)
            return inner

        both = jnp.where(jnp.logical_and(d >= 1, d <= 3), 2, 1)
        lax.fori_loop(0, both, one, 0)
        return carry

    lax.fori_loop(0, 5, turn, 0)

    for kv in range(2):
        copy(t, kv, 0, up).wait_send()
        copy(t, kv, 1, down).wait_send()
        copy(t, kv, 2, mate).wait_send()
        for d in range(1, 5):
            low, high = blocks(d)
            b_low, b_high = low * 2 + c, high * 2 + c
            copy(b_low, kv, 2, mate).wait_send()
            if d <= 3:
                copy(b_high, kv, 2, mate).wait_send()
            if d <= (3 if kv == 0 else 2):
                copy(b_low, kv, 0, up).wait_send()
            if d <= (3 if kv == 1 else 2):
                copy(b_high, kv, 1, down).wait_send()

    lane = lax.broadcasted_iota(jnp.int32, (rows_all, 128), 1)
    for pair in range(2):
        even, odd = acc_ref[2 * pair], acc_ref[2 * pair + 1]
        top = jnp.where(lane < HEAD, even, odd)
        total = pltpu.roll(jnp.where(lane < HEAD, odd, even), HEAD, 1)
        ctx_ref[:, 128 * pair : 128 * pair + 128] = (top / total).astype(BF16)


def attention(tokens, gain, weights):
    rows, width = tokens.shape
    n_tok = lax.axis_size("tok")
    local = weights.shape[2]
    vmem = pl.BlockSpec(memory_space=pltpu.VMEM)
    return pl.pallas_call(
        attention_kernel,
        out_shape=jax.ShapeDtypeStruct((rows, local), BF16),
        in_specs=[vmem] * 3,
        out_specs=vmem,
        scratch_shapes=[
            pltpu.VMEM((4, rows, 128), BF16),
            pltpu.VMEM((n_tok, 2, rows, local), BF16),
            pltpu.VMEM((4, 2 * rows, 128), BF16),
            pltpu.VMEM((4, rows, 128), F32),
            pltpu.VMEM((4, rows, 128), F32),
            pltpu.SemaphoreType.DMA((3, n_tok, 2)),
            pltpu.SemaphoreType.DMA((n_tok, 2)),
        ],
        compiler_params=pltpu.CompilerParams(
            collective_id=0, has_side_effects=True, vmem_limit_bytes=60 * 2**20
        ),
        name="attention",
    )(tokens, gain, weights)


RS_ROWS = 32
CG_TILES = 5
RS_CHUNKS = 14
CG_CHUNKS = 10


def pieces_of(value):
    high = value.astype(BF16)
    rest = value - high.astype(F32)
    mid = rest.astype(BF16)
    low = (rest - mid.astype(F32)).astype(BF16)
    return high, mid, low


def sigmoid(v):
    return 1.0 / (1.0 + jnp.exp(-v))


def network_kernel(
    ctx_ref,
    tok_ref,
    ow_ref,
    rwt_ref,
    cw_ref,
    cwt_ref,
    hw_ref,
    hwt_ref,
    cot_ref,
    holo_ref,
    cg_ref,
    og_ref,
    pbuf,
    ext,
    cbuf,
    st1,
    st2,
    sg,
    buf,
    rbuf,
    dbuf,
    fbuf,
    gbuf,
    p_send,
    p_recv,
    h_send,
    h_recv,
    s1,
    r1,
    s2,
    r2,
    s3,
    r3,
    s4,
    r4,
):
    t = lax.axis_index("tok")
    n_t = lax.axis_size("tok")
    dp = lax.axis_index("dp")
    n_dp = lax.axis_size("dp")
    col = lax.axis_index("col")
    other = 1 - col

    barrier = pltpu.get_barrier_semaphore()
    pl.semaphore_signal(barrier, inc=1, device_id={"col": other}, device_id_type=MESH)
    for k in range(1, n_t):
        pl.semaphore_signal(
            barrier, inc=1, device_id={"tok": lax.rem(t + k, n_t)}, device_id_type=MESH
        )
    for k in range(1, n_dp):
        pl.semaphore_signal(
            barrier, inc=1, device_id={"dp": lax.rem(dp + k, n_dp)}, device_id_type=MESH
        )

    high, mid, low = pieces_of(dot_nt(rwt_ref[...], ow_ref[...]))
    ctx = ctx_ref[...]
    pbuf[0] = dot_nt(high, ctx) + (dot_nt(mid, ctx) + dot_nt(low, ctx))
    cbuf[1, col] = cot_ref[...]
    pl.semaphore_wait(barrier, n_t + n_dp - 1)
    to_mate = {"col": other}
    c_copy = remote(cot_ref, cbuf.at[1, col], p_send.at[1], p_recv.at[1], to_mate)
    c_copy.start()
    p_copy = remote(pbuf.at[0], pbuf.at[1], p_send.at[0], p_recv.at[0], to_mate)
    p_copy.start()
    from_tokens = dot_nt(rwt_ref[...], tok_ref[...])
    p_copy.wait_recv()
    ext[2] = (from_tokens + (pbuf[0] + pbuf[1])).astype(BF16)
    c_copy.wait_recv()

    halo = []
    for k, (off, slot) in enumerate(((1, 1), (-1, 3), (2, 0), (-2, 4))):
        peer = {"tok": lax.rem(t + off + n_t, n_t)}
        halo.append(remote(ext.at[2], ext.at[slot], h_send.at[k], h_recv.at[k], peer))
        if k < 2:
            halo.append(
                remote(cbuf.at[1], cbuf.at[2 * k], h_send.at[4 + k], h_recv.at[4 + k], peer)
            )
    for item in halo:
        item.start()
    for item in halo:
        item.wait_recv()

    def in_frame(values, first_row):
        count = values.shape[1]
        row = lax.broadcasted_iota(jnp.int32, (1, count), 1) // 256 + (first_row - 4 + 2 * t)
        inside = jnp.logical_and(row >= 0, row < 2 * n_t)
        return jnp.where(inside, values, 0.0)

    def sides(values):
        count = values.shape[1]
        at = lax.broadcasted_iota(jnp.int32, (1, count), 1) % 256
        before = jnp.where(at == 0, 0.0, pltpu.roll(values, 1, 1))
        after = jnp.where(at == 255, 0.0, pltpu.roll(values, count - 1, 1))
        return before.astype(BF16), values.astype(BF16), after.astype(BF16)

    def stack(target, values, count, flip):
        shifted = sides(values)
        for a in range(3):
            for b in range(3):
                k = (3 * a + b) * 64
                row, piece = (2 - a, shifted[2 - b]) if flip else (a, shifted[b])
                target[k : k + 64, 0:count] = piece[:, row * 256 : row * 256 + count]

    x0 = in_frame(jnp.concatenate([ext[k].astype(F32) for k in range(5)], axis=1), 0)
    stack(st1, x0, 2048, False)
    pre1 = dot_nn(cw_ref[0], st1[...])
    sig1 = sigmoid(pre1)
    h1 = in_frame(pre1 * sig1, 1).astype(BF16)
    stack(st2, h1.astype(F32), 1536, False)
    pre2 = dot_nn(cw_ref[1], st2[...])
    sig2 = sigmoid(pre2)
    own2 = slice(512, 1024)
    h2 = (pre2[:, own2] * sig2[:, own2]).astype(BF16)
    holo = dot_nn(hw_ref[...], h2)
    for row in range(2):
        left = holo[:, row * 256 : row * 256 + 128]
        right = holo[:, row * 256 + 128 : row * 256 + 256]
        holo_ref[row] = jnp.where(col == 0, left, right)

    cot = jnp.concatenate(
        [cbuf[s, half, row] for s in range(3) for row in range(2) for half in range(2)], axis=1
    )
    gh2 = (hwt_ref[:, 0:1] * cot[0:1, :] + hwt_ref[:, 1:2] * cot[1:2, :]).astype(BF16)
    gp2 = in_frame(gh2.astype(F32) * sig2 * (1.0 + pre2 * (1.0 - sig2)), 2).astype(BF16)
    stack(sg, gp2.astype(F32), 1024, True)
    gh1 = dot_nn(cwt_ref[1], sg[...]).astype(BF16)
    sig1_in, pre1_in = sig1[:, 512:1536], pre1[:, 512:1536]
    gp1 = in_frame(gh1.astype(F32) * sig1_in * (1.0 + pre1_in * (1.0 - sig1_in)), 3).astype(BF16)
    stack(sg, gp1.astype(F32), 512, True)
    gh0 = dot_nn(cwt_ref[0], sg[:, 0:512]).astype(BF16)

    first = jnp.full((1, 1), col, jnp.int32) == 0
    grad = jnp.where(first, gp1[:, 256:768].astype(F32), gp2[:, own2].astype(F32)).astype(BF16)

    @pl.when(col == 0)
    def _():
        sg[:, 512:1024] = st1[:, 768:1280]

    @pl.when(col == 1)
    def _():
        sg[:, 512:1024] = st2[:, 512:1024]

    term = dot_nt(grad, sg[:, 512:1024])
    for k in range(4):
        buf[64 * k : 64 * k + 64, :] = term[:, 128 * k : 128 * k + 128]
    buf[256:320, 0:64] = term[:, 512:576]
    buf[256:320, 64:128] = jnp.zeros((64, 64), F32)
    small_term = dot_nn(gh0, ctx)
    buf[320:384, :] = small_term[:, 0:128]
    buf[384:448, :] = small_term[:, 128:256]

    def chunk(ref, i):
        return ref.at[pl.ds(pl.multiple_of(i * RS_ROWS, RS_ROWS), RS_ROWS), :]

    def phase1(k):
        peer = lax.rem(t + k, n_t)
        return peer, remote(chunk(buf, peer), rbuf.at[t], s1.at[k], r1.at[t], {"tok": peer})

    def arrival1(k):
        source = lax.rem(t + k, n_t)
        return remote(chunk(buf, 0), rbuf.at[source], s1.at[k], r1.at[source], {"tok": source})

    for k in range(1, n_t):
        peer, item = phase1(k)

        @pl.when(peer < RS_CHUNKS)
        def _():
            item.start()

    @pl.when(t < RS_CHUNKS)
    def _():
        rbuf[t] = buf[pl.ds(pl.multiple_of(t * RS_ROWS, RS_ROWS), RS_ROWS), :]
        for k in range(1, n_t):
            arrival1(k).wait_recv()
        total = rbuf[0]
        for j in range(1, n_t):
            total = total + rbuf[j]
        dbuf[dp] = total
        for k in range(1, n_dp):
            peer = lax.rem(dp + k, n_dp)
            remote(dbuf.at[dp], dbuf.at[dp], s2.at[k], r2.at[dp], {"dp": peer}).start()
        for k in range(1, n_dp):
            source = lax.rem(dp + k, n_dp)
            remote(
                dbuf.at[source], dbuf.at[source], s2.at[k], r2.at[source], {"dp": source}
            ).wait_recv()
        whole = dbuf[0]
        for j in range(1, n_dp):
            whole = whole + dbuf[j]
        fbuf[pl.ds(pl.multiple_of(t * RS_ROWS, RS_ROWS), RS_ROWS), :] = whole
        for k in range(1, n_t):
            peer = lax.rem(t + k, n_t)
            remote(chunk(fbuf, t), chunk(fbuf, t), s3.at[k], r3.at[t], {"tok": peer}).start()

    def cross(i):
        return remote(chunk(fbuf, i), chunk(gbuf, i), s4.at[i], r4.at[i], to_mate)

    for k in range(n_t):
        source = lax.rem(t + k, n_t)
        if k > 0:

            @pl.when(source < RS_CHUNKS)
            def _():
                remote(
                    chunk(fbuf, source), chunk(fbuf, source), s3.at[k], r3.at[source], {"tok": source}
                ).wait_recv()

        @pl.when(source < CG_CHUNKS)
        def _():
            cross(source).start()

    small = jnp.concatenate([fbuf[320:384, :], fbuf[384:448, :]], axis=1)
    small_t = jnp.transpose(small)
    parts = pieces_of(small_t)
    rwt = rwt_ref[...]
    og_ref[...] = dot_nn(parts[0], rwt) + (dot_nn(parts[1], rwt) + dot_nn(parts[2], rwt))

    for i in range(CG_CHUNKS):
        cross(i).wait_recv()
    for at, source in ((col, fbuf), (other, gbuf)):
        for k in range(4):
            cg_ref[at, :, 128 * k : 128 * k + 128] = source[64 * k : 64 * k + 64, :]
        cg_ref[at, :, 512:576] = source[256:320, 0:64]

    c_copy.wait_send()
    p_copy.wait_send()
    for item in halo:
        item.wait_send()
    for k in range(1, n_t):
        peer, item = phase1(k)

        @pl.when(peer < RS_CHUNKS)
        def _():
            item.wait_send()

    @pl.when(t < RS_CHUNKS)
    def _():
        for k in range(1, n_dp):
            peer = lax.rem(dp + k, n_dp)
            remote(dbuf.at[dp], dbuf.at[dp], s2.at[k], r2.at[dp], {"dp": peer}).wait_send()
        for k in range(1, n_t):
            peer = lax.rem(t + k, n_t)
            remote(chunk(fbuf, t), chunk(fbuf, t), s3.at[k], r3.at[t], {"tok": peer}).wait_send()

    for i in range(CG_CHUNKS):
        cross(i).wait_send()


def network(ctx, tokens, ow, rwt, cw, cwt, hw, hwt, cot):
    n_t, n_dp = lax.axis_size("tok"), lax.axis_size("dp")
    vmem = pl.BlockSpec(memory_space=pltpu.VMEM)
    dma = pltpu.SemaphoreType.DMA
    return pl.pallas_call(
        network_kernel,
        out_shape=(
            jax.ShapeDtypeStruct((2, 8, 128), F32),
            jax.ShapeDtypeStruct(cw.shape, F32),
            jax.ShapeDtypeStruct(ow.shape, F32),
        ),
        in_specs=[vmem] * 9,
        out_specs=(vmem,) * 3,
        scratch_shapes=[
            pltpu.VMEM((2, 64, 512), F32),
            pltpu.VMEM((5, 64, 512), BF16),
            pltpu.VMEM((3, 2, 2, 8, 128), F32),
            pltpu.VMEM((576, 2048), BF16),
            pltpu.VMEM((576, 1536), BF16),
            pltpu.VMEM((576, 1024), BF16),
            pltpu.VMEM((448, 128), F32),
            pltpu.VMEM((n_t, RS_ROWS, 128), F32),
            pltpu.VMEM((n_dp, RS_ROWS, 128), F32),
            pltpu.VMEM((448, 128), F32),
            pltpu.VMEM((320, 128), F32),
            dma((2,)),
            dma((2,)),
            dma((6,)),
            dma((6,)),
            dma((n_t,)),
            dma((n_t,)),
            dma((n_dp,)),
            dma((n_dp,)),
            dma((n_t,)),
            dma((n_t,)),
            dma((CG_CHUNKS,)),
            dma((CG_CHUNKS,)),
        ],
        compiler_params=pltpu.CompilerParams(
            collective_id=1, has_side_effects=True, vmem_limit_bytes=60 * 2**20
        ),
        name="network",
    )(ctx, tokens, ow, rwt, cw, cwt, hw, hwt, cot)


def transposed(weight):
    channels = weight.shape[0]
    return jnp.transpose(weight.reshape(channels, 9, channels), (2, 1, 0)).reshape(
        channels, 9 * channels
    )


def shards(
    tokens, ln_gain, qkv_weight, out_weight, readout_weight, conv_weight, head_weight, holo_cot
):
    rows_in = tokens[0]
    ctx = attention(rows_in, ln_gain.reshape(1, -1), qkv_weight)
    cwt = jnp.stack([transposed(conv_weight[k]) for k in range(2)])
    hw = jnp.pad(head_weight, ((0, 6), (0, 0)))
    hwt = jnp.pad(jnp.transpose(head_weight.astype(F32)), ((0, 0), (0, 126)))
    cot = jnp.pad(jnp.transpose(holo_cot[0], (1, 0, 2)), ((0, 0), (0, 6), (0, 0)))
    holo, conv_grad, out_grad = network(
        ctx, rows_in, out_weight, jnp.transpose(readout_weight), conv_weight, cwt, hw, hwt, cot
    )
    return (jnp.transpose(holo[:, 0:2], (1, 0, 2))[None], conv_grad, out_grad)


def solution(mesh):
    in_specs = (
        P("dp", "tok", None),
        P(),
        P(None, None, "col"),
        P("col", None),
        P(),
        P(),
        P(),
        P("dp", None, "tok", "col"),
    )
    out_specs = (P("dp", None, "tok", "col"), P(), P("col", None))
    return jax.shard_map(shards, mesh=mesh, in_specs=in_specs, out_specs=out_specs, check_vma=False)
```

```python
import functools

import jax
import jax.numpy as jnp
from jax import lax
from jax.experimental import pallas as pl
from jax.experimental.pallas import tpu as pltpu
from jax.sharding import PartitionSpec as P

HEAD = 64
EPSILON = 1e-05
MESH = pl.DeviceIdType.MESH
F32 = jnp.float32
BF16 = jnp.bfloat16

NT = (((1,), (1,)), ((), ()))


def dot_nt(a, b):
    return lax.dot_general(a, b, NT, preferred_element_type=F32)


def dot_nn(a, b):
    return jnp.dot(a, b, preferred_element_type=F32)


def remote(src, dst, send_sem, recv_sem, where):
    return pltpu.make_async_remote_copy(
        src_ref=src,
        dst_ref=dst,
        send_sem=send_sem,
        recv_sem=recv_sem,
        device_id=where,
        device_id_type=MESH,
    )


QT = 512
LN_ROWS = 128
KT = 512
HALF = 256


def low_lanes(shape):
    return lax.broadcasted_iota(jnp.int32, shape, 1) < HEAD


def swap_lanes(value):
    return pltpu.roll(value.astype(F32), HEAD, 1)


def attention_kernel(
    tok_ref,
    gain_ref,
    w_ref,
    ctx_ref,
    normed_ref,
    qout,
    qin,
    qz,
    kvout,
    kvb,
    vx,
    m_ref,
    acc_ref,
    oout,
    oin,
    q_send,
    q_recv,
    d_send,
    m_send,
    c_send,
    kv_recv,
    o_send,
    o_recv,
):
    t = lax.axis_index("tok")
    n_z = lax.axis_size("tok") // 2
    z, c = t // 2, lax.rem(t, 2)
    side = lax.rem(z, 2)
    head = z // 2
    step = 2 * side - 1

    def device(chip, core):
        return {"tok": chip * 2 + core}

    def source(i):
        return device(lax.rem(z + step * i + n_z, n_z), c)

    twin = device(z + 1 - 2 * side, c)
    mate = device(z, 1 - c)

    def target(far):
        way = step * (2 * (far % 2) - 1)
        return lax.rem(z + way * far + 2 * n_z, n_z)

    barrier = pltpu.get_barrier_semaphore()
    for k in range(1, 4):
        pl.semaphore_signal(barrier, inc=1, device_id=device(target(k), c), device_id_type=MESH)
        pl.semaphore_signal(barrier, inc=1, device_id=source(k), device_id_type=MESH)
    pl.semaphore_signal(barrier, inc=1, device_id=twin, device_id_type=MESH)
    pl.semaphore_signal(barrier, inc=1, device_id=mate, device_id_type=MESH)

    gain = gain_ref[...].astype(F32)
    low = low_lanes((LN_ROWS, 128))

    def both(r):
        first = pl.ds(pl.multiple_of(r * LN_ROWS, LN_ROWS), LN_ROWS)
        second = pl.ds(pl.multiple_of(HALF + r * LN_ROWS, LN_ROWS), LN_ROWS)
        return first, second

    def project_queries(r, carry):
        first, second = both(r)
        x = jnp.concatenate([tok_ref[first, :], tok_ref[second, :]], axis=0).astype(F32)
        center = x - jnp.mean(x, axis=-1, keepdims=True)
        spread = jnp.mean(center * center, axis=-1, keepdims=True)
        normed = (center * lax.rsqrt(spread + EPSILON) * gain).astype(BF16)
        normed_ref[first, :] = normed[0:LN_ROWS]
        normed_ref[second, :] = normed[LN_ROWS:]
        q = dot_nn(normed, w_ref[0])
        for pair in range(2):
            qt = q[:, 128 * pair : 128 * pair + 128]
            q_top, q_bottom = qt[0:LN_ROWS], qt[LN_ROWS:]
            qout[2 * pair, first, :] = jnp.where(low, q_top, swap_lanes(q_bottom)).astype(BF16)
            qout[2 * pair + 1, first, :] = jnp.where(low, swap_lanes(q_top), q_bottom).astype(BF16)
        return carry

    def project_keys(r, carry):
        first, second = both(r)
        normed = jnp.concatenate([normed_ref[first, :], normed_ref[second, :]], axis=0)
        k = dot_nn(normed, w_ref[1])
        v = dot_nn(normed, w_ref[2])
        for pair in range(2):
            tile = slice(128 * pair, 128 * pair + 128)
            kt, vt = k[:, tile], v[:, tile]
            v_moved, k_moved = swap_lanes(vt), swap_lanes(kt)
            for part, at in ((0, first), (1, second)):
                rows = slice(part * LN_ROWS, (part + 1) * LN_ROWS)
                kvout[2 * pair, at, :] = jnp.where(low, kt[rows], v_moved[rows]).astype(BF16)
                kvout[2 * pair + 1, at, :] = jnp.where(low, k_moved[rows], vt[rows]).astype(BF16)
        return carry

    def send_q(far):
        chip = target(far)
        return remote(
            qout.at[chip // 2], qin.at[far], q_send.at[far], q_recv.at[far], device(chip, c)
        )

    def send_kv(far):
        chip = target(far)
        return remote(
            kvout.at[chip // 2],
            kvb.at[2 * far, c],
            d_send.at[far],
            kv_recv.at[2 * far, c],
            device(chip, c),
        )

    def own(blk):
        return kvout.at[head] if blk == 0 else kvb.at[blk, c]

    def to_twin(i):
        there = 2 * i + 1
        return remote(own(2 * i), kvb.at[there, c], m_send.at[i], kv_recv.at[there, c], twin)

    def to_mate(blk):
        return remote(own(blk), kvb.at[blk, c], c_send.at[blk], kv_recv.at[blk, c], mate)

    def landed(blk, core):
        piece = kvb.at[blk, core]
        remote(piece, piece, c_send.at[blk], kv_recv.at[blk, core], mate).wait_recv()

    lax.fori_loop(0, HALF // LN_ROWS, project_queries, 0)
    pl.semaphore_wait(barrier, 8)
    for far in range(1, 4):
        send_q(far).start()
    lax.fori_loop(0, HALF // LN_ROWS, project_keys, 0)
    to_mate(0).start()
    to_twin(0).start()
    send_kv(1).start()
    kvb[0, c] = kvout[head]
    m_ref[...] = jnp.full(m_ref.shape, -1e30, F32)
    acc_ref[...] = jnp.zeros(acc_ref.shape, F32)

    low_h = low_lanes((HALF, 128))

    def unpack(packed):
        value = packed.astype(F32) * (1.0 / HEAD**0.5)
        top = jnp.where(low_h, value, 0.0).astype(BF16)
        bottom = jnp.where(low_h, pltpu.roll(value, HEAD, 1), 0.0).astype(BF16)
        return top, bottom

    def place(i, packed):
        top, bottom = unpack(packed)
        qz[i, 0:HALF, :] = top
        qz[i, HALF : 2 * HALF, :] = bottom

    place(0, qout[head])

    def take(blk, i, at_v):
        for tile in range(2 * HALF // QT):
            at = slice(tile * QT, (tile + 1) * QT)
            q = qz[i, at, :]
            s = [dot_nt(q, kvb[blk, half]) for half in range(2)]
            m_old = m_ref[i, at, :]
            top = jnp.maximum(
                jnp.max(s[0], axis=1, keepdims=True), jnp.max(s[1], axis=1, keepdims=True)
            )
            m_new = jnp.maximum(m_old, top)
            wide = jnp.concatenate([m_new] * (KT // 128), axis=1)
            out = None
            for half in range(2):
                p = jnp.exp(s[half] - wide).astype(BF16)
                o = dot_nn(p, vx[at_v, half])
                out = o if out is None else out + o
            acc_ref[i, at, :] = acc_ref[i, at, :] * jnp.exp(m_old - m_new) + out
            m_ref[i, at, :] = m_new

    def values(blk, at_v):
        low_k = low_lanes((KT, 128))
        for half in range(2):
            v = kvb[blk, half]
            vx[at_v, half] = jnp.where(low_k, jnp.ones_like(v), v)

    def send_o(i):
        return remote(oout.at[i], oin.at[head], o_send.at[i], o_recv.at[head], source(i))

    landed(0, 1 - c)
    values(0, 0)

    def first_block(i, carry):
        @pl.when(i > 0)
        def _():
            remote(qin.at[i], qin.at[i], q_send.at[0], q_recv.at[i], mate).wait_recv()
            top, bottom = unpack(qin[i])
            qz[i, 0:HALF, :] = top
            qz[i, HALF : 2 * HALF, :] = bottom

        take(0, i, 0)
        return carry

    lax.fori_loop(0, 4, first_block, 0)

    def relay(blk):
        landed(blk, c)
        remote(
            kvb.at[blk, c],
            kvb.at[blk + 1, c],
            m_send.at[blk // 2],
            kv_recv.at[blk + 1, c],
            twin,
        ).start()
        pass_on(blk)

    def pass_on(blk):
        remote(kvb.at[blk, c], kvb.at[blk, c], c_send.at[blk], kv_recv.at[blk, c], mate).start()

    def middle(blk, carry):
        @pl.when(blk == 1)
        def _():
            send_kv(2).start()

        @pl.when(blk == 2)
        def _():
            send_kv(3).start()

        @pl.when(lax.rem(blk, 2) == 1)
        def _():
            landed(blk, c)
            pass_on(blk)
            relay(jnp.minimum(blk + 1, 6))

        landed(blk, 1 - c)
        values(blk, 0)

        def each(i, inner):
            take(blk, i, 0)
            return inner

        lax.fori_loop(0, 4, each, 0)
        return carry

    lax.fori_loop(1, 6, middle, 0)

    landed(7, c)
    pass_on(7)
    for blk in (6, 7):
        landed(blk, 1 - c)
        values(blk, blk - 6)

    def last_blocks(j, carry):
        i = 3 - j

        def each(k, inner):
            take(6 + k, i, k)
            return inner

        lax.fori_loop(0, 2, each, 0)
        whole = acc_ref[i]
        done = whole / pltpu.roll(whole, HEAD, 1)
        packed = jnp.where(low_h, pltpu.roll(done[0:HALF], HEAD, 1), done[HALF:])
        oout[i] = packed.astype(BF16)

        @pl.when(i > 0)
        def _():
            send_o(i).start()

        return carry

    lax.fori_loop(0, 4, last_blocks, 0)
    oin[head] = oout[0]

    for k in range(1, 4):
        send_q(k).wait_send()
        send_kv(k).wait_send()
        send_o(k).wait_send()
    for i in range(4):
        to_twin(i).wait_send()
    for blk in range(8):
        to_mate(blk).wait_send()
    for k in range(1, 4):
        h = target(k) // 2
        remote(oin.at[h], oin.at[h], o_send.at[0], o_recv.at[h], mate).wait_recv()

    for pair in range(2):
        even, odd = oin[2 * pair].astype(F32), oin[2 * pair + 1].astype(F32)
        tile = slice(128 * pair, 128 * pair + 128)
        ctx_ref[0:HALF, tile] = jnp.where(low_h, even, pltpu.roll(odd, HEAD, 1)).astype(BF16)
        ctx_ref[HALF : 2 * HALF, tile] = jnp.where(low_h, pltpu.roll(even, HEAD, 1), odd).astype(BF16)


def attention(tokens, gain, weights):
    rows, width = tokens.shape
    n_tok = lax.axis_size("tok")
    local = weights.shape[2]
    vmem = pl.BlockSpec(memory_space=pltpu.VMEM)
    dma = pltpu.SemaphoreType.DMA
    return pl.pallas_call(
        attention_kernel,
        out_shape=jax.ShapeDtypeStruct((rows, local), BF16),
        in_specs=[vmem] * 3,
        out_specs=vmem,
        scratch_shapes=[
            pltpu.VMEM((rows, width), BF16),
            pltpu.VMEM((4, HALF, 128), BF16),
            pltpu.VMEM((4, HALF, 128), BF16),
            pltpu.VMEM((4, rows, 128), BF16),
            pltpu.VMEM((4, rows, 128), BF16),
            pltpu.VMEM((8, 2, rows, 128), BF16),
            pltpu.VMEM((2, 2, rows, 128), BF16),
            pltpu.VMEM((4, rows, 128), F32),
            pltpu.VMEM((4, rows, 128), F32),
            pltpu.VMEM((4, HALF, 128), BF16),
            pltpu.VMEM((4, HALF, 128), BF16),
            dma((4,)),
            dma((4,)),
            dma((4,)),
            dma((4,)),
            dma((8,)),
            dma((8, 2)),
            dma((4,)),
            dma((4,)),
        ],
        compiler_params=pltpu.CompilerParams(
            collective_id=0, has_side_effects=True, vmem_limit_bytes=60 * 2**20
        ),
        name="attention",
    )(tokens, gain, weights)


RS_ROWS = 32
CG_TILES = 5
RS_CHUNKS = 14
CG_CHUNKS = 10


def pieces_of(value):
    high = value.astype(BF16)
    rest = value - high.astype(F32)
    mid = rest.astype(BF16)
    low = (rest - mid.astype(F32)).astype(BF16)
    return high, mid, low


def sigmoid(v):
    return 1.0 / (1.0 + jnp.exp(-v))


def network_kernel(
    ctx_ref,
    tok_ref,
    ow_ref,
    rwt_ref,
    cw_ref,
    cwt_ref,
    hw_ref,
    hwt_ref,
    cot_ref,
    holo_ref,
    cg_ref,
    og_ref,
    pbuf,
    ext,
    cbuf,
    st1,
    st2,
    sg,
    buf,
    rbuf,
    dbuf,
    fbuf,
    gbuf,
    p_send,
    p_recv,
    h_send,
    h_recv,
    s1,
    r1,
    s2,
    r2,
    s3,
    r3,
    s4,
    r4,
):
    t = lax.axis_index("tok")
    n_t = lax.axis_size("tok")
    dp = lax.axis_index("dp")
    n_dp = lax.axis_size("dp")
    col = lax.axis_index("col")
    other = 1 - col

    barrier = pltpu.get_barrier_semaphore()
    pl.semaphore_signal(barrier, inc=1, device_id={"col": other}, device_id_type=MESH)
    for k in range(1, n_t):
        pl.semaphore_signal(
            barrier, inc=1, device_id={"tok": lax.rem(t + k, n_t)}, device_id_type=MESH
        )
    for k in range(1, n_dp):
        pl.semaphore_signal(
            barrier, inc=1, device_id={"dp": lax.rem(dp + k, n_dp)}, device_id_type=MESH
        )

    high, mid, low = pieces_of(dot_nt(rwt_ref[...], ow_ref[...]))
    ctx = ctx_ref[...]
    pbuf[0] = dot_nt(high, ctx) + (dot_nt(mid, ctx) + dot_nt(low, ctx))
    cbuf[1, col] = cot_ref[...]
    pl.semaphore_wait(barrier, n_t + n_dp - 1)
    to_mate = {"col": other}
    c_copy = remote(cot_ref, cbuf.at[1, col], p_send.at[1], p_recv.at[1], to_mate)
    c_copy.start()
    p_copy = remote(pbuf.at[0], pbuf.at[1], p_send.at[0], p_recv.at[0], to_mate)
    p_copy.start()
    from_tokens = dot_nt(rwt_ref[...], tok_ref[...])
    p_copy.wait_recv()
    ext[2] = (from_tokens + (pbuf[0] + pbuf[1])).astype(BF16)
    c_copy.wait_recv()

    halo = []
    for k, (off, slot) in enumerate(((1, 1), (-1, 3), (2, 0), (-2, 4))):
        peer = {"tok": lax.rem(t + off + n_t, n_t)}
        halo.append(remote(ext.at[2], ext.at[slot], h_send.at[k], h_recv.at[k], peer))
        if k < 2:
            halo.append(
                remote(cbuf.at[1], cbuf.at[2 * k], h_send.at[4 + k], h_recv.at[4 + k], peer)
            )
    for item in halo:
        item.start()
    for item in halo:
        item.wait_recv()

    def in_frame(values, first_row):
        count = values.shape[1]
        row = lax.broadcasted_iota(jnp.int32, (1, count), 1) // 256 + (first_row - 4 + 2 * t)
        inside = jnp.logical_and(row >= 0, row < 2 * n_t)
        return jnp.where(inside, values, 0.0)

    def sides(values):
        count = values.shape[1]
        at = lax.broadcasted_iota(jnp.int32, (1, count), 1) % 256
        before = jnp.where(at == 0, 0.0, pltpu.roll(values, 1, 1))
        after = jnp.where(at == 255, 0.0, pltpu.roll(values, count - 1, 1))
        return before.astype(BF16), values.astype(BF16), after.astype(BF16)

    def stack(target, values, count, flip):
        shifted = sides(values)
        for a in range(3):
            for b in range(3):
                k = (3 * a + b) * 64
                row, piece = (2 - a, shifted[2 - b]) if flip else (a, shifted[b])
                target[k : k + 64, 0:count] = piece[:, row * 256 : row * 256 + count]

    x0 = in_frame(jnp.concatenate([ext[k].astype(F32) for k in range(5)], axis=1), 0)
    stack(st1, x0, 2048, False)
    pre1 = dot_nn(cw_ref[0], st1[...])
    sig1 = sigmoid(pre1)
    h1 = in_frame(pre1 * sig1, 1).astype(BF16)
    stack(st2, h1.astype(F32), 1536, False)
    pre2 = dot_nn(cw_ref[1], st2[...])
    sig2 = sigmoid(pre2)
    own2 = slice(512, 1024)
    h2 = (pre2[:, own2] * sig2[:, own2]).astype(BF16)
    holo = dot_nn(hw_ref[...], h2)
    for row in range(2):
        left = holo[:, row * 256 : row * 256 + 128]
        right = holo[:, row * 256 + 128 : row * 256 + 256]
        holo_ref[row] = jnp.where(col == 0, left, right)

    cot = jnp.concatenate(
        [cbuf[s, half, row] for s in range(3) for row in range(2) for half in range(2)], axis=1
    )
    gh2 = (hwt_ref[:, 0:1] * cot[0:1, :] + hwt_ref[:, 1:2] * cot[1:2, :]).astype(BF16)
    gp2 = in_frame(gh2.astype(F32) * sig2 * (1.0 + pre2 * (1.0 - sig2)), 2).astype(BF16)
    stack(sg, gp2.astype(F32), 1024, True)
    gh1 = dot_nn(cwt_ref[1], sg[...]).astype(BF16)
    sig1_in, pre1_in = sig1[:, 512:1536], pre1[:, 512:1536]
    gp1 = in_frame(gh1.astype(F32) * sig1_in * (1.0 + pre1_in * (1.0 - sig1_in)), 3).astype(BF16)
    stack(sg, gp1.astype(F32), 512, True)
    gh0 = dot_nn(cwt_ref[0], sg[:, 0:512]).astype(BF16)

    first = jnp.full((1, 1), col, jnp.int32) == 0
    grad = jnp.where(first, gp1[:, 256:768].astype(F32), gp2[:, own2].astype(F32)).astype(BF16)

    @pl.when(col == 0)
    def _():
        sg[:, 512:1024] = st1[:, 768:1280]

    @pl.when(col == 1)
    def _():
        sg[:, 512:1024] = st2[:, 512:1024]

    term = dot_nt(grad, sg[:, 512:1024])
    for k in range(4):
        buf[64 * k : 64 * k + 64, :] = term[:, 128 * k : 128 * k + 128]
    buf[256:320, 0:64] = term[:, 512:576]
    buf[256:320, 64:128] = jnp.zeros((64, 64), F32)
    small_term = dot_nn(gh0, ctx)
    buf[320:384, :] = small_term[:, 0:128]
    buf[384:448, :] = small_term[:, 128:256]

    def chunk(ref, i):
        return ref.at[pl.ds(pl.multiple_of(i * RS_ROWS, RS_ROWS), RS_ROWS), :]

    def phase1(k):
        peer = lax.rem(t + k, n_t)
        return peer, remote(chunk(buf, peer), rbuf.at[t], s1.at[k], r1.at[t], {"tok": peer})

    def arrival1(k):
        source = lax.rem(t + k, n_t)
        return remote(chunk(buf, 0), rbuf.at[source], s1.at[k], r1.at[source], {"tok": source})

    for k in range(1, n_t):
        peer, item = phase1(k)

        @pl.when(peer < RS_CHUNKS)
        def _():
            item.start()

    @pl.when(t < RS_CHUNKS)
    def _():
        rbuf[t] = buf[pl.ds(pl.multiple_of(t * RS_ROWS, RS_ROWS), RS_ROWS), :]
        for k in range(1, n_t):
            arrival1(k).wait_recv()
        total = rbuf[0]
        for j in range(1, n_t):
            total = total + rbuf[j]
        dbuf[dp] = total
        for k in range(1, n_dp):
            peer = lax.rem(dp + k, n_dp)
            remote(dbuf.at[dp], dbuf.at[dp], s2.at[k], r2.at[dp], {"dp": peer}).start()
        for k in range(1, n_dp):
            source = lax.rem(dp + k, n_dp)
            remote(
                dbuf.at[source], dbuf.at[source], s2.at[k], r2.at[source], {"dp": source}
            ).wait_recv()
        whole = dbuf[0]
        for j in range(1, n_dp):
            whole = whole + dbuf[j]
        fbuf[pl.ds(pl.multiple_of(t * RS_ROWS, RS_ROWS), RS_ROWS), :] = whole
        for k in range(1, n_t):
            peer = lax.rem(t + k, n_t)
            remote(chunk(fbuf, t), chunk(fbuf, t), s3.at[k], r3.at[t], {"tok": peer}).start()

    def cross(i):
        return remote(chunk(fbuf, i), chunk(gbuf, i), s4.at[i], r4.at[i], to_mate)

    for k in range(n_t):
        source = lax.rem(t + k, n_t)
        if k > 0:

            @pl.when(source < RS_CHUNKS)
            def _():
                remote(
                    chunk(fbuf, source), chunk(fbuf, source), s3.at[k], r3.at[source], {"tok": source}
                ).wait_recv()

        @pl.when(source < CG_CHUNKS)
        def _():
            cross(source).start()

    small = jnp.concatenate([fbuf[320:384, :], fbuf[384:448, :]], axis=1)
    small_t = jnp.transpose(small)
    parts = pieces_of(small_t)
    rwt = rwt_ref[...]
    og_ref[...] = dot_nn(parts[0], rwt) + (dot_nn(parts[1], rwt) + dot_nn(parts[2], rwt))

    for i in range(CG_CHUNKS):
        cross(i).wait_recv()
    for at, source in ((col, fbuf), (other, gbuf)):
        for k in range(4):
            cg_ref[at, :, 128 * k : 128 * k + 128] = source[64 * k : 64 * k + 64, :]
        cg_ref[at, :, 512:576] = source[256:320, 0:64]

    c_copy.wait_send()
    p_copy.wait_send()
    for item in halo:
        item.wait_send()
    for k in range(1, n_t):
        peer, item = phase1(k)

        @pl.when(peer < RS_CHUNKS)
        def _():
            item.wait_send()

    @pl.when(t < RS_CHUNKS)
    def _():
        for k in range(1, n_dp):
            peer = lax.rem(dp + k, n_dp)
            remote(dbuf.at[dp], dbuf.at[dp], s2.at[k], r2.at[dp], {"dp": peer}).wait_send()
        for k in range(1, n_t):
            peer = lax.rem(t + k, n_t)
            remote(chunk(fbuf, t), chunk(fbuf, t), s3.at[k], r3.at[t], {"tok": peer}).wait_send()

    for i in range(CG_CHUNKS):
        cross(i).wait_send()


def network(ctx, tokens, ow, rwt, cw, cwt, hw, hwt, cot):
    n_t, n_dp = lax.axis_size("tok"), lax.axis_size("dp")
    vmem = pl.BlockSpec(memory_space=pltpu.VMEM)
    dma = pltpu.SemaphoreType.DMA
    return pl.pallas_call(
        network_kernel,
        out_shape=(
            jax.ShapeDtypeStruct((2, 8, 128), F32),
            jax.ShapeDtypeStruct(cw.shape, F32),
            jax.ShapeDtypeStruct(ow.shape, F32),
        ),
        in_specs=[vmem] * 9,
        out_specs=(vmem,) * 3,
        scratch_shapes=[
            pltpu.VMEM((2, 64, 512), F32),
            pltpu.VMEM((5, 64, 512), BF16),
            pltpu.VMEM((3, 2, 2, 8, 128), F32),
            pltpu.VMEM((576, 2048), BF16),
            pltpu.VMEM((576, 1536), BF16),
            pltpu.VMEM((576, 1024), BF16),
            pltpu.VMEM((448, 128), F32),
            pltpu.VMEM((n_t, RS_ROWS, 128), F32),
            pltpu.VMEM((n_dp, RS_ROWS, 128), F32),
            pltpu.VMEM((448, 128), F32),
            pltpu.VMEM((320, 128), F32),
            dma((2,)),
            dma((2,)),
            dma((6,)),
            dma((6,)),
            dma((n_t,)),
            dma((n_t,)),
            dma((n_dp,)),
            dma((n_dp,)),
            dma((n_t,)),
            dma((n_t,)),
            dma((CG_CHUNKS,)),
            dma((CG_CHUNKS,)),
        ],
        compiler_params=pltpu.CompilerParams(
            collective_id=1, has_side_effects=True, vmem_limit_bytes=60 * 2**20
        ),
        name="network",
    )(ctx, tokens, ow, rwt, cw, cwt, hw, hwt, cot)


def transposed(weight):
    channels = weight.shape[0]
    return jnp.transpose(weight.reshape(channels, 9, channels), (2, 1, 0)).reshape(
        channels, 9 * channels
    )


def shards(
    tokens, ln_gain, qkv_weight, out_weight, readout_weight, conv_weight, head_weight, holo_cot
):
    rows_in = tokens[0]
    ctx = attention(rows_in, ln_gain.reshape(1, -1), qkv_weight)
    cwt = jnp.stack([transposed(conv_weight[k]) for k in range(2)])
    hw = jnp.pad(head_weight, ((0, 6), (0, 0)))
    hwt = jnp.pad(jnp.transpose(head_weight.astype(F32)), ((0, 0), (0, 126)))
    cot = jnp.pad(jnp.transpose(holo_cot[0], (1, 0, 2)), ((0, 0), (0, 6), (0, 0)))
    holo, conv_grad, out_grad = network(
        ctx, rows_in, out_weight, jnp.transpose(readout_weight), conv_weight, cwt, hw, hwt, cot
    )
    return (jnp.transpose(holo[:, 0:2], (1, 0, 2))[None], conv_grad, out_grad)


def solution(mesh):
    in_specs = (
        P("dp", "tok", None),
        P(),
        P(None, None, "col"),
        P("col", None),
        P(),
        P(),
        P(),
        P("dp", None, "tok", "col"),
    )
    out_specs = (P("dp", None, "tok", "col"), P(), P("col", None))
    return jax.shard_map(shards, mesh=mesh, in_specs=in_specs, out_specs=out_specs, check_vma=False)
```

```python
import functools

import jax
import jax.numpy as jnp
from jax import lax
from jax.experimental import pallas as pl
from jax.experimental.pallas import tpu as pltpu
from jax.sharding import PartitionSpec as P

HEAD = 64
EPSILON = 1e-05
MESH = pl.DeviceIdType.MESH
F32 = jnp.float32
BF16 = jnp.bfloat16

NT = (((1,), (1,)), ((), ()))


def dot_nt(a, b):
    return lax.dot_general(a, b, NT, preferred_element_type=F32)


def dot_nn(a, b):
    return jnp.dot(a, b, preferred_element_type=F32)


def remote(src, dst, send_sem, recv_sem, where):
    return pltpu.make_async_remote_copy(
        src_ref=src,
        dst_ref=dst,
        send_sem=send_sem,
        recv_sem=recv_sem,
        device_id=where,
        device_id_type=MESH,
    )


QT = 512
LN_ROWS = 128
KT = 512
HALF = 256


def low_lanes(shape):
    return lax.broadcasted_iota(jnp.int32, shape, 1) < HEAD


def swap_lanes(value):
    return pltpu.roll(value.astype(F32), HEAD, 1)


def attention_kernel(
    tok_ref,
    gain_ref,
    w_ref,
    ctx_ref,
    normed_ref,
    qout,
    qin,
    qz,
    kvout,
    kvb,
    vx,
    m_ref,
    acc_ref,
    oout,
    oin,
    q_send,
    q_recv,
    d_send,
    m_send,
    c_send,
    kv_recv,
    o_send,
    o_recv,
):
    t = lax.axis_index("tok")
    n_z = lax.axis_size("tok") // 2
    z, c = t // 2, lax.rem(t, 2)
    side = lax.rem(z, 2)
    head = z // 2
    step = 2 * side - 1

    def device(chip, core):
        return {"tok": chip * 2 + core}

    def source(i):
        return device(lax.rem(z + step * i + n_z, n_z), c)

    twin = device(z + 1 - 2 * side, c)
    mate = device(z, 1 - c)

    def target(far):
        way = step * (2 * (far % 2) - 1)
        return lax.rem(z + way * far + 2 * n_z, n_z)

    barrier = pltpu.get_barrier_semaphore()
    for k in range(1, 4):
        pl.semaphore_signal(barrier, inc=1, device_id=device(target(k), c), device_id_type=MESH)
        pl.semaphore_signal(barrier, inc=1, device_id=source(k), device_id_type=MESH)
    pl.semaphore_signal(barrier, inc=1, device_id=twin, device_id_type=MESH)
    pl.semaphore_signal(barrier, inc=1, device_id=mate, device_id_type=MESH)

    gain = gain_ref[...].astype(F32).reshape(1, -1)
    low = low_lanes((LN_ROWS, 128))

    def both(r):
        first = pl.ds(pl.multiple_of(r * LN_ROWS, LN_ROWS), LN_ROWS)
        second = pl.ds(pl.multiple_of(HALF + r * LN_ROWS, LN_ROWS), LN_ROWS)
        return first, second

    def project_queries(r, carry):
        first, second = both(r)
        x = jnp.concatenate([tok_ref[first, :], tok_ref[second, :]], axis=0).astype(F32)
        center = x - jnp.mean(x, axis=-1, keepdims=True)
        spread = jnp.mean(center * center, axis=-1, keepdims=True)
        normed = (center * lax.rsqrt(spread + EPSILON) * gain).astype(BF16)
        normed_ref[first, :] = normed[0:LN_ROWS]
        normed_ref[second, :] = normed[LN_ROWS:]
        q = dot_nn(normed, w_ref[0])
        for pair in range(2):
            qt = q[:, 128 * pair : 128 * pair + 128]
            q_top, q_bottom = qt[0:LN_ROWS], qt[LN_ROWS:]
            qout[2 * pair, first, :] = jnp.where(low, q_top, swap_lanes(q_bottom)).astype(BF16)
            qout[2 * pair + 1, first, :] = jnp.where(low, swap_lanes(q_top), q_bottom).astype(BF16)
        return carry

    def project_keys(r, carry):
        first, second = both(r)
        normed = jnp.concatenate([normed_ref[first, :], normed_ref[second, :]], axis=0)
        k = dot_nn(normed, w_ref[1])
        v = dot_nn(normed, w_ref[2])
        for pair in range(2):
            tile = slice(128 * pair, 128 * pair + 128)
            kt, vt = k[:, tile], v[:, tile]
            v_moved, k_moved = swap_lanes(vt), swap_lanes(kt)
            for part, at in ((0, first), (1, second)):
                rows = slice(part * LN_ROWS, (part + 1) * LN_ROWS)
                kvout[2 * pair, at, :] = jnp.where(low, kt[rows], v_moved[rows]).astype(BF16)
                kvout[2 * pair + 1, at, :] = jnp.where(low, k_moved[rows], vt[rows]).astype(BF16)
        return carry

    def send_q(far):
        chip = target(far)
        return remote(
            qout.at[chip // 2], qin.at[far], q_send.at[far], q_recv.at[far], device(chip, c)
        )

    def send_kv(far):
        chip = target(far)
        return remote(
            kvout.at[chip // 2],
            kvb.at[2 * far, c],
            d_send.at[far],
            kv_recv.at[2 * far, c],
            device(chip, c),
        )

    def own(blk):
        return kvout.at[head] if blk == 0 else kvb.at[blk, c]

    def to_twin(i):
        there = 2 * i + 1
        return remote(own(2 * i), kvb.at[there, c], m_send.at[i], kv_recv.at[there, c], twin)

    def to_mate(blk):
        return remote(own(blk), kvb.at[blk, c], c_send.at[blk], kv_recv.at[blk, c], mate)

    def landed(blk, core):
        piece = kvb.at[blk, core]
        remote(piece, piece, c_send.at[blk], kv_recv.at[blk, core], mate).wait_recv()

    lax.fori_loop(0, HALF // LN_ROWS, project_queries, 0)
    pl.semaphore_wait(barrier, 8)
    for far in range(1, 4):
        send_q(far).start()
    lax.fori_loop(0, HALF // LN_ROWS, project_keys, 0)
    to_mate(0).start()
    to_twin(0).start()
    send_kv(1).start()
    kvb[0, c] = kvout[head]
    m_ref[...] = jnp.full(m_ref.shape, -1e30, F32)
    acc_ref[...] = jnp.zeros(acc_ref.shape, F32)

    low_h = low_lanes((HALF, 128))

    def unpack(packed):
        value = packed.astype(F32) * (1.0 / HEAD**0.5)
        top = jnp.where(low_h, value, 0.0).astype(BF16)
        bottom = jnp.where(low_h, pltpu.roll(value, HEAD, 1), 0.0).astype(BF16)
        return top, bottom

    def place(i, packed):
        top, bottom = unpack(packed)
        qz[i, 0:HALF, :] = top
        qz[i, HALF : 2 * HALF, :] = bottom

    place(0, qout[head])

    def take(blk, i, at_v):
        for tile in range(2 * HALF // QT):
            at = slice(tile * QT, (tile + 1) * QT)
            q = qz[i, at, :]
            s = [dot_nt(q, kvb[blk, half]) for half in range(2)]
            m_old = m_ref[i, at, :]
            top = jnp.maximum(
                jnp.max(s[0], axis=1, keepdims=True), jnp.max(s[1], axis=1, keepdims=True)
            )
            m_new = jnp.maximum(m_old, top)
            wide = jnp.concatenate([m_new] * (KT // 128), axis=1)
            out = None
            for half in range(2):
                p = jnp.exp(s[half] - wide).astype(BF16)
                o = dot_nn(p, vx[at_v, half])
                out = o if out is None else out + o
            acc_ref[i, at, :] = acc_ref[i, at, :] * jnp.exp(m_old - m_new) + out
            m_ref[i, at, :] = m_new

    def values(blk, at_v):
        low_k = low_lanes((KT, 128))
        for half in range(2):
            v = kvb[blk, half]
            vx[at_v, half] = jnp.where(low_k, jnp.ones_like(v), v)

    def send_o(i):
        return remote(oout.at[i], oin.at[head], o_send.at[i], o_recv.at[head], source(i))

    landed(0, 1 - c)
    values(0, 0)

    def first_block(i, carry):
        @pl.when(i > 0)
        def _():
            remote(qin.at[i], qin.at[i], q_send.at[0], q_recv.at[i], mate).wait_recv()
            top, bottom = unpack(qin[i])
            qz[i, 0:HALF, :] = top
            qz[i, HALF : 2 * HALF, :] = bottom

        take(0, i, 0)
        return carry

    lax.fori_loop(0, 4, first_block, 0)

    def relay(blk):
        landed(blk, c)
        remote(
            kvb.at[blk, c],
            kvb.at[blk + 1, c],
            m_send.at[blk // 2],
            kv_recv.at[blk + 1, c],
            twin,
        ).start()
        pass_on(blk)

    def pass_on(blk):
        remote(kvb.at[blk, c], kvb.at[blk, c], c_send.at[blk], kv_recv.at[blk, c], mate).start()

    def middle(blk, carry):
        @pl.when(blk == 1)
        def _():
            send_kv(2).start()

        @pl.when(blk == 2)
        def _():
            send_kv(3).start()

        @pl.when(lax.rem(blk, 2) == 1)
        def _():
            landed(blk, c)
            pass_on(blk)
            relay(jnp.minimum(blk + 1, 6))

        landed(blk, 1 - c)
        values(blk, 0)

        def each(i, inner):
            take(blk, i, 0)
            return inner

        lax.fori_loop(0, 4, each, 0)
        return carry

    lax.fori_loop(1, 6, middle, 0)

    landed(7, c)
    pass_on(7)
    for blk in (6, 7):
        landed(blk, 1 - c)
        values(blk, blk - 6)

    def last_blocks(j, carry):
        i = 3 - j

        def each(k, inner):
            take(6 + k, i, k)
            return inner

        lax.fori_loop(0, 2, each, 0)
        whole = acc_ref[i]
        done = whole / pltpu.roll(whole, HEAD, 1)
        packed = jnp.where(low_h, pltpu.roll(done[0:HALF], HEAD, 1), done[HALF:])
        oout[i] = packed.astype(BF16)

        @pl.when(i > 0)
        def _():
            send_o(i).start()

        return carry

    lax.fori_loop(0, 4, last_blocks, 0)
    oin[head] = oout[0]

    for k in range(1, 4):
        send_q(k).wait_send()
        send_kv(k).wait_send()
        send_o(k).wait_send()
    for i in range(4):
        to_twin(i).wait_send()
    for blk in range(8):
        to_mate(blk).wait_send()
    for k in range(1, 4):
        h = target(k) // 2
        remote(oin.at[h], oin.at[h], o_send.at[0], o_recv.at[h], mate).wait_recv()

    for pair in range(2):
        even, odd = oin[2 * pair].astype(F32), oin[2 * pair + 1].astype(F32)
        tile = slice(128 * pair, 128 * pair + 128)
        ctx_ref[0:HALF, tile] = jnp.where(low_h, even, pltpu.roll(odd, HEAD, 1)).astype(BF16)
        ctx_ref[HALF : 2 * HALF, tile] = jnp.where(low_h, pltpu.roll(even, HEAD, 1), odd).astype(BF16)


def attention(tokens, gain, weights):
    rows, width = tokens.shape
    n_tok = lax.axis_size("tok")
    local = weights.shape[2]
    vmem = pl.BlockSpec(memory_space=pltpu.VMEM)
    dma = pltpu.SemaphoreType.DMA
    return pl.pallas_call(
        attention_kernel,
        out_shape=jax.ShapeDtypeStruct((rows, local), BF16),
        in_specs=[vmem] * 3,
        out_specs=vmem,
        scratch_shapes=[
            pltpu.VMEM((rows, width), BF16),
            pltpu.VMEM((4, HALF, 128), BF16),
            pltpu.VMEM((4, HALF, 128), BF16),
            pltpu.VMEM((4, rows, 128), BF16),
            pltpu.VMEM((4, rows, 128), BF16),
            pltpu.VMEM((8, 2, rows, 128), BF16),
            pltpu.VMEM((2, 2, rows, 128), BF16),
            pltpu.VMEM((4, rows, 128), F32),
            pltpu.VMEM((4, rows, 128), F32),
            pltpu.VMEM((4, HALF, 128), BF16),
            pltpu.VMEM((4, HALF, 128), BF16),
            dma((4,)),
            dma((4,)),
            dma((4,)),
            dma((4,)),
            dma((8,)),
            dma((8, 2)),
            dma((4,)),
            dma((4,)),
        ],
        compiler_params=pltpu.CompilerParams(
            collective_id=0, has_side_effects=True, vmem_limit_bytes=60 * 2**20
        ),
        name="attention",
    )(tokens, gain, weights)


RS_ROWS = 32
CG_TILES = 5
RS_CHUNKS = 14
CG_CHUNKS = 10


def pieces_of(value):
    high = value.astype(BF16)
    rest = value - high.astype(F32)
    mid = rest.astype(BF16)
    low = (rest - mid.astype(F32)).astype(BF16)
    return high, mid, low


def sigmoid(v):
    return 1.0 / (1.0 + jnp.exp(-v))


def network_kernel(
    ctx_ref,
    tok_ref,
    ow_ref,
    rwt_ref,
    cw_ref,
    hw_ref,
    cot_ref,
    holo_ref,
    own_ref,
    other_ref,
    cwt_ref,
    pbuf,
    ext,
    cbuf,
    st1,
    st2,
    sg,
    buf,
    rbuf,
    dbuf,
    fbuf,
    gbuf,
    p_send,
    p_recv,
    h_send,
    h_recv,
    s1,
    r1,
    s2,
    r2,
    s3,
    r3,
    s4,
    r4,
):
    t = lax.axis_index("tok")
    n_t = lax.axis_size("tok")
    dp = lax.axis_index("dp")
    n_dp = lax.axis_size("dp")
    col = lax.axis_index("col")
    other = 1 - col

    barrier = pltpu.get_barrier_semaphore()
    pl.semaphore_signal(barrier, inc=1, device_id={"col": other}, device_id_type=MESH)
    for k in range(1, n_t):
        pl.semaphore_signal(
            barrier, inc=1, device_id={"tok": lax.rem(t + k, n_t)}, device_id_type=MESH
        )
    for k in range(1, n_dp):
        pl.semaphore_signal(
            barrier, inc=1, device_id={"dp": lax.rem(dp + k, n_dp)}, device_id_type=MESH
        )

    high, mid, low = pieces_of(dot_nt(rwt_ref[...], ow_ref[...]))
    ctx = ctx_ref[...]
    pbuf[0] = dot_nt(high, ctx) + (dot_nt(mid, ctx) + dot_nt(low, ctx))
    cbuf[1, col] = cot_ref[...]
    pl.semaphore_wait(barrier, n_t + n_dp - 1)
    to_mate = {"col": other}
    c_copy = remote(cot_ref, cbuf.at[1, col], p_send.at[1], p_recv.at[1], to_mate)
    p_copy = remote(pbuf.at[0], pbuf.at[1], p_send.at[0], p_recv.at[0], to_mate)
    p_copy.start()
    c_copy.start()
    from_tokens = dot_nt(rwt_ref[...], tok_ref[...])
    for layer in range(2):
        for k in range(9):
            tap = slice(64 * k, 64 * k + 64)
            turned = jnp.transpose(cw_ref[layer, :, tap].astype(F32))
            cwt_ref[layer, :, tap] = turned.astype(BF16)
    p_copy.wait_recv()
    ext[2] = (from_tokens + (pbuf[0] + pbuf[1])).astype(BF16)
    c_copy.wait_recv()

    halo = []
    for k, (off, slot) in enumerate(((1, 1), (-1, 3), (2, 0), (-2, 4))):
        peer = {"tok": lax.rem(t + off + n_t, n_t)}
        halo.append(remote(ext.at[2], ext.at[slot], h_send.at[k], h_recv.at[k], peer))
        if k < 2:
            halo.append(
                remote(cbuf.at[1], cbuf.at[2 * k], h_send.at[4 + k], h_recv.at[4 + k], peer)
            )
    for item in halo:
        item.start()
    for item in halo:
        item.wait_recv()

    def in_frame(values, first_row):
        count = values.shape[1]
        row = lax.broadcasted_iota(jnp.int32, (1, count), 1) // 256 + (first_row - 4 + 2 * t)
        inside = jnp.logical_and(row >= 0, row < 2 * n_t)
        return jnp.where(inside, values, 0.0)

    def sides(values):
        count = values.shape[1]
        at = lax.broadcasted_iota(jnp.int32, (1, count), 1) % 256
        before = jnp.where(at == 0, 0.0, pltpu.roll(values, 1, 1))
        after = jnp.where(at == 255, 0.0, pltpu.roll(values, count - 1, 1))
        return before.astype(BF16), values.astype(BF16), after.astype(BF16)

    def stack(target, values, count, flip):
        shifted = sides(values)
        for a in range(3):
            for b in range(3):
                k = (3 * a + b) * 64
                row, piece = (2 - a, shifted[2 - b]) if flip else (a, shifted[b])
                target[k : k + 64, 0:count] = piece[:, row * 256 : row * 256 + count]

    x0 = in_frame(jnp.concatenate([ext[k].astype(F32) for k in range(5)], axis=1), 0)
    stack(st1, x0, 2048, False)
    pre1 = dot_nn(cw_ref[0], st1[...])
    sig1 = sigmoid(pre1)
    h1 = in_frame(pre1 * sig1, 1).astype(BF16)
    stack(st2, h1.astype(F32), 1536, False)
    pre2 = dot_nn(cw_ref[1], st2[...])
    sig2 = sigmoid(pre2)
    own2 = slice(512, 1024)
    h2 = (pre2[:, own2] * sig2[:, own2]).astype(BF16)
    holo = dot_nn(hw_ref[...], h2)
    for row in range(2):
        left = holo[:, row * 256 : row * 256 + 128]
        right = holo[:, row * 256 + 128 : row * 256 + 256]
        holo_ref[:, row, :] = jnp.where(col == 0, left, right)

    diagonal = lax.broadcasted_iota(jnp.int32, (64, 64), 0) == lax.broadcasted_iota(
        jnp.int32, (64, 64), 1
    )
    raised = None
    for k in range(2):
        cot = jnp.concatenate(
            [
                cbuf[s, half, k, row : row + 1, :]
                for s in range(3)
                for row in range(2)
                for half in range(2)
            ],
            axis=1,
        )
        weight = jnp.where(diagonal, hw_ref[k : k + 1, :].astype(F32), 0.0)
        product = jnp.sum(weight, axis=1, keepdims=True) * cot
        raised = product if raised is None else raised + product
    gh2 = raised.astype(BF16)
    gp2 = in_frame(gh2.astype(F32) * sig2 * (1.0 + pre2 * (1.0 - sig2)), 2).astype(BF16)
    stack(sg, gp2.astype(F32), 1024, True)
    gh1 = dot_nn(cwt_ref[1], sg[...]).astype(BF16)
    sig1_in, pre1_in = sig1[:, 512:1536], pre1[:, 512:1536]
    gp1 = in_frame(gh1.astype(F32) * sig1_in * (1.0 + pre1_in * (1.0 - sig1_in)), 3).astype(BF16)
    stack(sg, gp1.astype(F32), 512, True)
    gh0 = dot_nn(cwt_ref[0], sg[:, 0:512]).astype(BF16)

    first = jnp.full((1, 1), col, jnp.int32) == 0
    grad = jnp.where(first, gp1[:, 256:768].astype(F32), gp2[:, own2].astype(F32)).astype(BF16)

    @pl.when(col == 0)
    def _():
        sg[:, 512:1024] = st1[:, 768:1280]

    @pl.when(col == 1)
    def _():
        sg[:, 512:1024] = st2[:, 512:1024]

    term = dot_nt(grad, sg[:, 512:1024])
    for k in range(4):
        buf[64 * k : 64 * k + 64, :] = term[:, 128 * k : 128 * k + 128]
    buf[256:320, 0:64] = term[:, 512:576]
    buf[256:320, 64:128] = jnp.zeros((64, 64), F32)
    small_term = dot_nn(gh0, ctx)
    buf[320:384, :] = small_term[:, 0:128]
    buf[384:448, :] = small_term[:, 128:256]

    def chunk(ref, i):
        return ref.at[pl.ds(pl.multiple_of(i * RS_ROWS, RS_ROWS), RS_ROWS), :]

    def phase1(k):
        peer = lax.rem(t + k, n_t)
        return peer, remote(chunk(buf, peer), rbuf.at[t], s1.at[k], r1.at[t], {"tok": peer})

    def arrival1(k):
        source = lax.rem(t + k, n_t)
        return remote(chunk(buf, 0), rbuf.at[source], s1.at[k], r1.at[source], {"tok": source})

    for k in range(1, n_t):
        peer, item = phase1(k)

        @pl.when(peer < RS_CHUNKS)
        def _():
            item.start()

    @pl.when(t < RS_CHUNKS)
    def _():
        rbuf[t] = buf[pl.ds(pl.multiple_of(t * RS_ROWS, RS_ROWS), RS_ROWS), :]
        for k in range(1, n_t):
            arrival1(k).wait_recv()
        total = rbuf[0]
        for j in range(1, n_t):
            total = total + rbuf[j]
        dbuf[dp] = total
        for k in range(1, n_dp):
            peer = lax.rem(dp + k, n_dp)
            remote(dbuf.at[dp], dbuf.at[dp], s2.at[k], r2.at[dp], {"dp": peer}).start()
        for k in range(1, n_dp):
            source = lax.rem(dp + k, n_dp)
            remote(
                dbuf.at[source], dbuf.at[source], s2.at[k], r2.at[source], {"dp": source}
            ).wait_recv()
        whole = dbuf[0]
        for j in range(1, n_dp):
            whole = whole + dbuf[j]
        fbuf[pl.ds(pl.multiple_of(t * RS_ROWS, RS_ROWS), RS_ROWS), :] = whole.astype(BF16)
        for k in range(1, n_t):
            peer = lax.rem(t + k, n_t)
            remote(chunk(fbuf, t), chunk(fbuf, t), s3.at[k], r3.at[t], {"tok": peer}).start()

    def cross(i):
        return remote(chunk(fbuf, i), chunk(gbuf, i), s4.at[i], r4.at[i], to_mate)

    for k in sorted(range(n_t), key=lambda k: min(k, n_t - k)):
        source = lax.rem(t + k, n_t)
        if k > 0:

            @pl.when(source < RS_CHUNKS)
            def _():
                remote(
                    chunk(fbuf, source), chunk(fbuf, source), s3.at[k], r3.at[source], {"tok": source}
                ).wait_recv()

        @pl.when(source < CG_CHUNKS)
        def _():
            cross(source).start()

    own_ref[...] = fbuf[...]
    for i in range(CG_CHUNKS):
        cross(i).wait_recv()
    other_ref[...] = gbuf[...]

    c_copy.wait_send()
    p_copy.wait_send()
    for item in halo:
        item.wait_send()
    for k in range(1, n_t):
        peer, item = phase1(k)

        @pl.when(peer < RS_CHUNKS)
        def _():
            item.wait_send()

    @pl.when(t < RS_CHUNKS)
    def _():
        for k in range(1, n_dp):
            peer = lax.rem(dp + k, n_dp)
            remote(dbuf.at[dp], dbuf.at[dp], s2.at[k], r2.at[dp], {"dp": peer}).wait_send()
        for k in range(1, n_t):
            peer = lax.rem(t + k, n_t)
            remote(chunk(fbuf, t), chunk(fbuf, t), s3.at[k], r3.at[t], {"tok": peer}).wait_send()

    for i in range(CG_CHUNKS):
        cross(i).wait_send()


def network(ctx, tokens, ow, rwt, cw, hw, cot):
    n_t, n_dp = lax.axis_size("tok"), lax.axis_size("dp")
    vmem = pl.BlockSpec(memory_space=pltpu.VMEM)
    dma = pltpu.SemaphoreType.DMA
    return pl.pallas_call(
        network_kernel,
        out_shape=(
            jax.ShapeDtypeStruct(cot.shape, F32),
            jax.ShapeDtypeStruct((448, 128), BF16),
            jax.ShapeDtypeStruct((320, 128), BF16),
        ),
        in_specs=[vmem] * 7,
        out_specs=(vmem,) * 3,
        scratch_shapes=[
            pltpu.VMEM((2, 64, 576), BF16),
            pltpu.VMEM((2, 64, 512), F32),
            pltpu.VMEM((5, 64, 512), BF16),
            pltpu.VMEM((3, 2, 2, 2, 128), F32),
            pltpu.VMEM((576, 2048), BF16),
            pltpu.VMEM((576, 1536), BF16),
            pltpu.VMEM((576, 1024), BF16),
            pltpu.VMEM((448, 128), F32),
            pltpu.VMEM((n_t, RS_ROWS, 128), F32),
            pltpu.VMEM((n_dp, RS_ROWS, 128), F32),
            pltpu.VMEM((448, 128), BF16),
            pltpu.VMEM((320, 128), BF16),
            dma((2,)),
            dma((2,)),
            dma((6,)),
            dma((6,)),
            dma((n_t,)),
            dma((n_t,)),
            dma((n_dp,)),
            dma((n_dp,)),
            dma((n_t,)),
            dma((n_t,)),
            dma((CG_CHUNKS,)),
            dma((CG_CHUNKS,)),
        ],
        compiler_params=pltpu.CompilerParams(
            collective_id=1, has_side_effects=True, vmem_limit_bytes=60 * 2**20
        ),
        name="network",
    )(ctx, tokens, ow, rwt, cw, hw, cot)


def finish_kernel(holo_in, own_ref, other_ref, rwt_ref, holo_ref, cg_ref, og_ref):
    col = lax.axis_index("col")
    small = jnp.concatenate([own_ref[320:384, :], own_ref[384:448, :]], axis=1)
    og_ref[...] = dot_nn(jnp.transpose(small.astype(F32)).astype(BF16), rwt_ref[...])
    for at, source in ((col, own_ref), (1 - col, other_ref)):
        for k in range(4):
            cg_ref[at, :, 128 * k : 128 * k + 128] = source[64 * k : 64 * k + 64, :].astype(F32)
        cg_ref[at, :, 512:576] = source[256:320, 0:64].astype(F32)
    holo_ref[0] = holo_in[...]


def finish(holo, own, other, rwt, cw, ow):
    vmem = pl.BlockSpec(memory_space=pltpu.VMEM)
    return pl.pallas_call(
        finish_kernel,
        out_shape=(
            jax.ShapeDtypeStruct((1, *holo.shape), F32),
            jax.ShapeDtypeStruct(cw.shape, F32),
            jax.ShapeDtypeStruct(ow.shape, F32),
        ),
        in_specs=[vmem] * 4,
        out_specs=(vmem,) * 3,
        name="finish",
    )(holo, own, other, rwt)


def shards(
    tokens, ln_gain, qkv_weight, out_weight, readout_weight, conv_weight, head_weight, holo_cot
):
    rows_in = tokens[0]
    ctx = attention(rows_in, ln_gain, qkv_weight)
    rwt = jnp.transpose(readout_weight)
    holo, own, other = network(
        ctx, rows_in, out_weight, rwt, conv_weight, head_weight, holo_cot[0]
    )
    return finish(holo, own, other, rwt, conv_weight, out_weight)


def solution(mesh):
    in_specs = (
        P("dp", "tok", None),
        P(),
        P(None, None, "col"),
        P("col", None),
        P(),
        P(),
        P(),
        P("dp", None, "tok", "col"),
    )
    out_specs = (P("dp", None, "tok", "col"), P(), P("col", None))
    return jax.shard_map(shards, mesh=mesh, in_specs=in_specs, out_specs=out_specs, check_vma=False)
```

```python
import functools

import jax
import jax.numpy as jnp
from jax import lax
from jax.experimental import pallas as pl
from jax.experimental.pallas import tpu as pltpu
from jax.sharding import PartitionSpec as P

HEAD = 64
EPSILON = 1e-05
MESH = pl.DeviceIdType.MESH
F32 = jnp.float32
BF16 = jnp.bfloat16

NT = (((1,), (1,)), ((), ()))


def dot_nt(a, b):
    return lax.dot_general(a, b, NT, preferred_element_type=F32)


def dot_nn(a, b):
    return jnp.dot(a, b, preferred_element_type=F32)


def remote(src, dst, send_sem, recv_sem, where):
    return pltpu.make_async_remote_copy(
        src_ref=src,
        dst_ref=dst,
        send_sem=send_sem,
        recv_sem=recv_sem,
        device_id=where,
        device_id_type=MESH,
    )


QT = 512
LN_ROWS = 128
KT = 512
HALF = 256


def low_lanes(shape):
    return lax.broadcasted_iota(jnp.int32, shape, 1) < HEAD


def swap_lanes(value):
    return pltpu.roll(value.astype(F32), HEAD, 1)


def attention_part(
    ready,
    meanwhile,
    tok_ref,
    gain_ref,
    w_ref,
    ctx_ref,
    normed_ref,
    qout,
    qin,
    qz,
    kvout,
    kvb,
    vx,
    m_ref,
    acc_ref,
    oout,
    oin,
    q_send,
    q_recv,
    d_send,
    m_send,
    c_send,
    kv_recv,
    o_send,
    o_recv,
):
    t = lax.axis_index("tok")
    n_z = lax.axis_size("tok") // 2
    z, c = t // 2, lax.rem(t, 2)
    side = lax.rem(z, 2)
    head = z // 2
    step = 2 * side - 1

    def device(chip, core):
        return {"tok": chip * 2 + core}

    def source(i):
        return device(lax.rem(z + step * i + n_z, n_z), c)

    twin = device(z + 1 - 2 * side, c)
    mate = device(z, 1 - c)

    def target(far):
        way = step * (2 * (far % 2) - 1)
        return lax.rem(z + way * far + 2 * n_z, n_z)

    gain = gain_ref[...].astype(F32).reshape(1, -1)
    low = low_lanes((LN_ROWS, 128))

    def both(r):
        first = pl.ds(pl.multiple_of(r * LN_ROWS, LN_ROWS), LN_ROWS)
        second = pl.ds(pl.multiple_of(HALF + r * LN_ROWS, LN_ROWS), LN_ROWS)
        return first, second

    def project_queries(r, carry):
        first, second = both(r)
        x = jnp.concatenate([tok_ref[first, :], tok_ref[second, :]], axis=0).astype(F32)
        center = x - jnp.mean(x, axis=-1, keepdims=True)
        spread = jnp.mean(center * center, axis=-1, keepdims=True)
        normed = (center * lax.rsqrt(spread + EPSILON) * gain).astype(BF16)
        normed_ref[first, :] = normed[0:LN_ROWS]
        normed_ref[second, :] = normed[LN_ROWS:]
        q = dot_nn(normed, w_ref[0])
        for pair in range(2):
            qt = q[:, 128 * pair : 128 * pair + 128]
            q_top, q_bottom = qt[0:LN_ROWS], qt[LN_ROWS:]
            qout[2 * pair, first, :] = jnp.where(low, q_top, swap_lanes(q_bottom)).astype(BF16)
            qout[2 * pair + 1, first, :] = jnp.where(low, swap_lanes(q_top), q_bottom).astype(BF16)
        return carry

    def project_keys(r, carry):
        first, second = both(r)
        normed = jnp.concatenate([normed_ref[first, :], normed_ref[second, :]], axis=0)
        k = dot_nn(normed, w_ref[1])
        v = dot_nn(normed, w_ref[2])
        for pair in range(2):
            tile = slice(128 * pair, 128 * pair + 128)
            kt, vt = k[:, tile], v[:, tile]
            v_moved, k_moved = swap_lanes(vt), swap_lanes(kt)
            for part, at in ((0, first), (1, second)):
                rows = slice(part * LN_ROWS, (part + 1) * LN_ROWS)
                kvout[2 * pair, at, :] = jnp.where(low, kt[rows], v_moved[rows]).astype(BF16)
                kvout[2 * pair + 1, at, :] = jnp.where(low, k_moved[rows], vt[rows]).astype(BF16)
        return carry

    def send_q(far):
        chip = target(far)
        return remote(
            qout.at[chip // 2], qin.at[far], q_send.at[far], q_recv.at[far], device(chip, c)
        )

    def send_kv(far):
        chip = target(far)
        return remote(
            kvout.at[chip // 2],
            kvb.at[2 * far, c],
            d_send.at[far],
            kv_recv.at[2 * far, c],
            device(chip, c),
        )

    def own(blk):
        return kvout.at[head] if blk == 0 else kvb.at[blk, c]

    def to_twin(i):
        there = 2 * i + 1
        return remote(own(2 * i), kvb.at[there, c], m_send.at[i], kv_recv.at[there, c], twin)

    def to_mate(blk):
        return remote(own(blk), kvb.at[blk, c], c_send.at[blk], kv_recv.at[blk, c], mate)

    def landed(blk, core):
        piece = kvb.at[blk, core]
        remote(piece, piece, c_send.at[blk], kv_recv.at[blk, core], mate).wait_recv()

    lax.fori_loop(0, HALF // LN_ROWS, project_queries, 0)
    ready()
    for far in range(1, 4):
        send_q(far).start()
    lax.fori_loop(0, HALF // LN_ROWS, project_keys, 0)
    to_mate(0).start()
    to_twin(0).start()
    send_kv(1).start()
    kvb[0, c] = kvout[head]
    meanwhile()
    m_ref[...] = jnp.full(m_ref.shape, -1e30, F32)
    acc_ref[...] = jnp.zeros(acc_ref.shape, F32)

    low_h = low_lanes((HALF, 128))

    def unpack(packed):
        value = packed.astype(F32) * (1.0 / HEAD**0.5)
        top = jnp.where(low_h, value, 0.0).astype(BF16)
        bottom = jnp.where(low_h, pltpu.roll(value, HEAD, 1), 0.0).astype(BF16)
        return top, bottom

    def place(i, packed):
        top, bottom = unpack(packed)
        qz[i, 0:HALF, :] = top
        qz[i, HALF : 2 * HALF, :] = bottom

    place(0, qout[head])

    def take(blk, i, at_v):
        for tile in range(2 * HALF // QT):
            at = slice(tile * QT, (tile + 1) * QT)
            q = qz[i, at, :]
            s = [dot_nt(q, kvb[blk, half]) for half in range(2)]
            m_old = m_ref[i, at, :]
            top = jnp.maximum(
                jnp.max(s[0], axis=1, keepdims=True), jnp.max(s[1], axis=1, keepdims=True)
            )
            m_new = jnp.maximum(m_old, top)
            wide = jnp.concatenate([m_new] * (KT // 128), axis=1)
            out = None
            for half in range(2):
                p = jnp.exp(s[half] - wide).astype(BF16)
                o = dot_nn(p, vx[at_v, half])
                out = o if out is None else out + o
            acc_ref[i, at, :] = acc_ref[i, at, :] * jnp.exp(m_old - m_new) + out
            m_ref[i, at, :] = m_new

    def values(blk, at_v):
        low_k = low_lanes((KT, 128))
        for half in range(2):
            v = kvb[blk, half]
            vx[at_v, half] = jnp.where(low_k, jnp.ones_like(v), v)

    def send_o(i):
        return remote(oout.at[i], oin.at[head], o_send.at[i], o_recv.at[head], source(i))

    landed(0, 1 - c)
    values(0, 0)

    def first_block(i, carry):
        @pl.when(i > 0)
        def _():
            remote(qin.at[i], qin.at[i], q_send.at[0], q_recv.at[i], mate).wait_recv()
            top, bottom = unpack(qin[i])
            qz[i, 0:HALF, :] = top
            qz[i, HALF : 2 * HALF, :] = bottom

        take(0, i, 0)
        return carry

    lax.fori_loop(0, 4, first_block, 0)

    def relay(blk):
        landed(blk, c)
        remote(
            kvb.at[blk, c],
            kvb.at[blk + 1, c],
            m_send.at[blk // 2],
            kv_recv.at[blk + 1, c],
            twin,
        ).start()
        pass_on(blk)

    def pass_on(blk):
        remote(kvb.at[blk, c], kvb.at[blk, c], c_send.at[blk], kv_recv.at[blk, c], mate).start()

    def middle(blk, carry):
        @pl.when(blk == 1)
        def _():
            send_kv(2).start()

        @pl.when(blk == 2)
        def _():
            send_kv(3).start()

        @pl.when(lax.rem(blk, 2) == 1)
        def _():
            landed(blk, c)
            pass_on(blk)
            relay(jnp.minimum(blk + 1, 6))

        landed(blk, 1 - c)
        values(blk, 0)

        def each(i, inner):
            take(blk, i, 0)
            return inner

        lax.fori_loop(0, 4, each, 0)
        return carry

    lax.fori_loop(1, 6, middle, 0)

    landed(7, c)
    pass_on(7)
    for blk in (6, 7):
        landed(blk, 1 - c)
        values(blk, blk - 6)

    def last_blocks(j, carry):
        i = 3 - j

        def each(k, inner):
            take(6 + k, i, k)
            return inner

        lax.fori_loop(0, 2, each, 0)
        whole = acc_ref[i]
        done = whole / pltpu.roll(whole, HEAD, 1)
        packed = jnp.where(low_h, pltpu.roll(done[0:HALF], HEAD, 1), done[HALF:])
        oout[i] = packed.astype(BF16)

        @pl.when(i > 0)
        def _():
            send_o(i).start()

        return carry

    lax.fori_loop(0, 4, last_blocks, 0)
    oin[head] = oout[0]

    for k in range(1, 4):
        send_q(k).wait_send()
        send_kv(k).wait_send()
        send_o(k).wait_send()
    for i in range(4):
        to_twin(i).wait_send()
    for blk in range(8):
        to_mate(blk).wait_send()
    for k in range(1, 4):
        h = target(k) // 2
        remote(oin.at[h], oin.at[h], o_send.at[0], o_recv.at[h], mate).wait_recv()

    for pair in range(2):
        even, odd = oin[2 * pair].astype(F32), oin[2 * pair + 1].astype(F32)
        tile = slice(128 * pair, 128 * pair + 128)
        ctx_ref[0:HALF, tile] = jnp.where(low_h, even, pltpu.roll(odd, HEAD, 1)).astype(BF16)
        ctx_ref[HALF : 2 * HALF, tile] = jnp.where(low_h, pltpu.roll(even, HEAD, 1), odd).astype(BF16)


RS_ROWS = 32
CG_TILES = 5
RS_CHUNKS = 14
CG_CHUNKS = 10


def pieces_of(value):
    high = value.astype(BF16)
    rest = value - high.astype(F32)
    mid = rest.astype(BF16)
    low = (rest - mid.astype(F32)).astype(BF16)
    return high, mid, low


def sigmoid(v):
    return 1.0 / (1.0 + jnp.exp(-v))


def step_kernel(
    tok_ref,
    gain_ref,
    w_ref,
    ow_ref,
    rwt_ref,
    cw_ref,
    hw_ref,
    cot_ref,
    holo_ref,
    own_ref,
    other_ref,
    ctx_ref,
    w2_ref,
    base_ref,
    cwt_ref,
    pbuf,
    ext,
    cbuf,
    st1,
    st2,
    sg,
    buf,
    rbuf,
    dbuf,
    fbuf,
    gbuf,
    p_send,
    p_recv,
    h_send,
    h_recv,
    s1,
    r1,
    s2,
    r2,
    s3,
    r3,
    s4,
    r4,
    *attention_refs,
):
    t = lax.axis_index("tok")
    n_t = lax.axis_size("tok")
    dp = lax.axis_index("dp")
    n_dp = lax.axis_size("dp")
    col = lax.axis_index("col")
    other = 1 - col

    barrier = pltpu.get_barrier_semaphore()
    pl.semaphore_signal(barrier, inc=1, device_id={"col": other}, device_id_type=MESH)
    for k in range(1, n_t):
        pl.semaphore_signal(
            barrier, inc=1, device_id={"tok": lax.rem(t + k, n_t)}, device_id_type=MESH
        )
    for k in range(1, n_dp):
        pl.semaphore_signal(
            barrier, inc=1, device_id={"dp": lax.rem(dp + k, n_dp)}, device_id_type=MESH
        )

    to_mate = {"col": other}
    c_copy = remote(cot_ref, cbuf.at[1, col], p_send.at[1], p_recv.at[1], to_mate)

    def ready():
        pl.semaphore_wait(barrier, n_t + n_dp - 1)

    def meanwhile():
        c_copy.start()
        cbuf[1, col] = cot_ref[...]
        for k, piece in enumerate(pieces_of(dot_nt(rwt_ref[...], ow_ref[...]))):
            w2_ref[k] = piece
        base_ref[...] = dot_nt(rwt_ref[...], tok_ref[...])
        for layer in range(2):
            for k in range(9):
                tap = slice(64 * k, 64 * k + 64)
                turned = jnp.transpose(cw_ref[layer, :, tap].astype(F32))
                cwt_ref[layer, :, tap] = turned.astype(BF16)

    attention_part(ready, meanwhile, tok_ref, gain_ref, w_ref, ctx_ref, *attention_refs)

    ctx = ctx_ref[...]
    pbuf[0] = dot_nt(w2_ref[0], ctx) + (dot_nt(w2_ref[1], ctx) + dot_nt(w2_ref[2], ctx))
    p_copy = remote(pbuf.at[0], pbuf.at[1], p_send.at[0], p_recv.at[0], to_mate)
    p_copy.start()
    p_copy.wait_recv()
    ext[2] = (base_ref[...] + (pbuf[0] + pbuf[1])).astype(BF16)
    c_copy.wait_recv()

    halo = []
    for k, (off, slot) in enumerate(((1, 1), (-1, 3), (2, 0), (-2, 4))):
        peer = {"tok": lax.rem(t + off + n_t, n_t)}
        halo.append(remote(ext.at[2], ext.at[slot], h_send.at[k], h_recv.at[k], peer))
        if k < 2:
            halo.append(
                remote(cbuf.at[1], cbuf.at[2 * k], h_send.at[4 + k], h_recv.at[4 + k], peer)
            )
    for item in halo:
        item.start()
    for item in halo:
        item.wait_recv()

    def in_frame(values, first_row):
        count = values.shape[1]
        row = lax.broadcasted_iota(jnp.int32, (1, count), 1) // 256 + (first_row - 4 + 2 * t)
        inside = jnp.logical_and(row >= 0, row < 2 * n_t)
        return jnp.where(inside, values, 0.0)

    def sides(values):
        count = values.shape[1]
        at = lax.broadcasted_iota(jnp.int32, (1, count), 1) % 256
        before = jnp.where(at == 0, 0.0, pltpu.roll(values, 1, 1))
        after = jnp.where(at == 255, 0.0, pltpu.roll(values, count - 1, 1))
        return before.astype(BF16), values.astype(BF16), after.astype(BF16)

    def stack(target, values, count, flip):
        shifted = sides(values)
        for a in range(3):
            for b in range(3):
                k = (3 * a + b) * 64
                row, piece = (2 - a, shifted[2 - b]) if flip else (a, shifted[b])
                target[k : k + 64, 0:count] = piece[:, row * 256 : row * 256 + count]

    x0 = in_frame(jnp.concatenate([ext[k].astype(F32) for k in range(5)], axis=1), 0)
    stack(st1, x0, 2048, False)
    pre1 = dot_nn(cw_ref[0], st1[...])
    sig1 = sigmoid(pre1)
    h1 = in_frame(pre1 * sig1, 1).astype(BF16)
    stack(st2, h1.astype(F32), 1536, False)
    pre2 = dot_nn(cw_ref[1], st2[...])
    sig2 = sigmoid(pre2)
    own2 = slice(512, 1024)
    h2 = (pre2[:, own2] * sig2[:, own2]).astype(BF16)
    holo = dot_nn(hw_ref[...], h2)
    for row in range(2):
        left = holo[:, row * 256 : row * 256 + 128]
        right = holo[:, row * 256 + 128 : row * 256 + 256]
        holo_ref[:, row, :] = jnp.where(col == 0, left, right)

    diagonal = lax.broadcasted_iota(jnp.int32, (64, 64), 0) == lax.broadcasted_iota(
        jnp.int32, (64, 64), 1
    )
    raised = None
    for k in range(2):
        cot = jnp.concatenate(
            [
                cbuf[s, half, k, row : row + 1, :]
                for s in range(3)
                for row in range(2)
                for half in range(2)
            ],
            axis=1,
        )
        weight = jnp.where(diagonal, hw_ref[k : k + 1, :].astype(F32), 0.0)
        product = jnp.sum(weight, axis=1, keepdims=True) * cot
        raised = product if raised is None else raised + product
    gh2 = raised.astype(BF16)
    gp2 = in_frame(gh2.astype(F32) * sig2 * (1.0 + pre2 * (1.0 - sig2)), 2).astype(BF16)
    stack(sg, gp2.astype(F32), 1024, True)
    gh1 = dot_nn(cwt_ref[1], sg[...]).astype(BF16)
    sig1_in, pre1_in = sig1[:, 512:1536], pre1[:, 512:1536]
    gp1 = in_frame(gh1.astype(F32) * sig1_in * (1.0 + pre1_in * (1.0 - sig1_in)), 3).astype(BF16)
    stack(sg, gp1.astype(F32), 512, True)
    gh0 = dot_nn(cwt_ref[0], sg[:, 0:512]).astype(BF16)

    first = jnp.full((1, 1), col, jnp.int32) == 0
    grad = jnp.where(first, gp1[:, 256:768].astype(F32), gp2[:, own2].astype(F32)).astype(BF16)

    @pl.when(col == 0)
    def _():
        sg[:, 512:1024] = st1[:, 768:1280]

    @pl.when(col == 1)
    def _():
        sg[:, 512:1024] = st2[:, 512:1024]

    term = dot_nt(grad, sg[:, 512:1024])
    for k in range(4):
        buf[64 * k : 64 * k + 64, :] = term[:, 128 * k : 128 * k + 128].astype(BF16)
    buf[256:320, 0:64] = term[:, 512:576].astype(BF16)
    buf[256:320, 64:128] = jnp.zeros((64, 64), BF16)
    small_term = dot_nn(gh0, ctx)
    buf[320:384, :] = small_term[:, 0:128].astype(BF16)
    buf[384:448, :] = small_term[:, 128:256].astype(BF16)

    def chunk(ref, i):
        return ref.at[pl.ds(pl.multiple_of(i * RS_ROWS, RS_ROWS), RS_ROWS), :]

    def phase1(k):
        peer = lax.rem(t + k, n_t)
        return peer, remote(chunk(buf, peer), rbuf.at[t], s1.at[k], r1.at[t], {"tok": peer})

    def arrival1(k):
        source = lax.rem(t + k, n_t)
        return remote(chunk(buf, 0), rbuf.at[source], s1.at[k], r1.at[source], {"tok": source})

    for k in range(1, n_t):
        peer, item = phase1(k)

        @pl.when(peer < RS_CHUNKS)
        def _():
            item.start()

    @pl.when(t < RS_CHUNKS)
    def _():
        rbuf[t] = buf[pl.ds(pl.multiple_of(t * RS_ROWS, RS_ROWS), RS_ROWS), :]
        for k in range(1, n_t):
            arrival1(k).wait_recv()
        total = rbuf[0].astype(F32)
        for j in range(1, n_t):
            total = total + rbuf[j].astype(F32)
        dbuf[dp] = total
        for k in range(1, n_dp):
            peer = lax.rem(dp + k, n_dp)
            remote(dbuf.at[dp], dbuf.at[dp], s2.at[k], r2.at[dp], {"dp": peer}).start()
        for k in range(1, n_dp):
            source = lax.rem(dp + k, n_dp)
            remote(
                dbuf.at[source], dbuf.at[source], s2.at[k], r2.at[source], {"dp": source}
            ).wait_recv()
        whole = dbuf[0]
        for j in range(1, n_dp):
            whole = whole + dbuf[j]
        fbuf[pl.ds(pl.multiple_of(t * RS_ROWS, RS_ROWS), RS_ROWS), :] = whole.astype(BF16)
        for k in range(1, n_t):
            peer = lax.rem(t + k, n_t)
            remote(chunk(fbuf, t), chunk(fbuf, t), s3.at[k], r3.at[t], {"tok": peer}).start()

    def cross(i):
        return remote(chunk(fbuf, i), chunk(gbuf, i), s4.at[i], r4.at[i], to_mate)

    for k in sorted(range(n_t), key=lambda k: min(k, n_t - k)):
        source = lax.rem(t + k, n_t)
        if k > 0:

            @pl.when(source < RS_CHUNKS)
            def _():
                remote(
                    chunk(fbuf, source), chunk(fbuf, source), s3.at[k], r3.at[source], {"tok": source}
                ).wait_recv()

        @pl.when(source < CG_CHUNKS)
        def _():
            cross(source).start()

    own_ref[...] = fbuf[...]
    for i in range(CG_CHUNKS):
        cross(i).wait_recv()
    other_ref[...] = gbuf[...]

    c_copy.wait_send()
    p_copy.wait_send()
    for item in halo:
        item.wait_send()
    for k in range(1, n_t):
        peer, item = phase1(k)

        @pl.when(peer < RS_CHUNKS)
        def _():
            item.wait_send()

    @pl.when(t < RS_CHUNKS)
    def _():
        for k in range(1, n_dp):
            peer = lax.rem(dp + k, n_dp)
            remote(dbuf.at[dp], dbuf.at[dp], s2.at[k], r2.at[dp], {"dp": peer}).wait_send()
        for k in range(1, n_t):
            peer = lax.rem(t + k, n_t)
            remote(chunk(fbuf, t), chunk(fbuf, t), s3.at[k], r3.at[t], {"tok": peer}).wait_send()

    for i in range(CG_CHUNKS):
        cross(i).wait_send()


def step(tokens, gain, weights, ow, rwt, cw, hw, cot):
    rows, width = tokens.shape
    n_tok = lax.axis_size("tok")
    local = weights.shape[2]
    n_t, n_dp = lax.axis_size("tok"), lax.axis_size("dp")
    vmem = pl.BlockSpec(memory_space=pltpu.VMEM)
    dma = pltpu.SemaphoreType.DMA
    return pl.pallas_call(
        step_kernel,
        out_shape=(
            jax.ShapeDtypeStruct(cot.shape, F32),
            jax.ShapeDtypeStruct((448, 128), BF16),
            jax.ShapeDtypeStruct((320, 128), BF16),
        ),
        in_specs=[vmem] * 8,
        out_specs=(vmem,) * 3,
        scratch_shapes=[
            pltpu.VMEM((rows, local), BF16),
            pltpu.VMEM((3, 64, local), BF16),
            pltpu.VMEM((64, rows), F32),
            pltpu.VMEM((2, 64, 576), BF16),
            pltpu.VMEM((2, 64, 512), F32),
            pltpu.VMEM((5, 64, 512), BF16),
            pltpu.VMEM((3, 2, 2, 2, 128), F32),
            pltpu.VMEM((576, 2048), BF16),
            pltpu.VMEM((576, 1536), BF16),
            pltpu.VMEM((576, 1024), BF16),
            pltpu.VMEM((448, 128), BF16),
            pltpu.VMEM((n_t, RS_ROWS, 128), BF16),
            pltpu.VMEM((n_dp, RS_ROWS, 128), F32),
            pltpu.VMEM((448, 128), BF16),
            pltpu.VMEM((320, 128), BF16),
            dma((2,)),
            dma((2,)),
            dma((6,)),
            dma((6,)),
            dma((n_t,)),
            dma((n_t,)),
            dma((n_dp,)),
            dma((n_dp,)),
            dma((n_t,)),
            dma((n_t,)),
            dma((CG_CHUNKS,)),
            dma((CG_CHUNKS,)),
            pltpu.VMEM((rows, width), BF16),
            pltpu.VMEM((4, HALF, 128), BF16),
            pltpu.VMEM((4, HALF, 128), BF16),
            pltpu.VMEM((4, rows, 128), BF16),
            pltpu.VMEM((4, rows, 128), BF16),
            pltpu.VMEM((8, 2, rows, 128), BF16),
            pltpu.VMEM((2, 2, rows, 128), BF16),
            pltpu.VMEM((4, rows, 128), F32),
            pltpu.VMEM((4, rows, 128), F32),
            pltpu.VMEM((4, HALF, 128), BF16),
            pltpu.VMEM((4, HALF, 128), BF16),
            dma((4,)),
            dma((4,)),
            dma((4,)),
            dma((4,)),
            dma((8,)),
            dma((8, 2)),
            dma((4,)),
            dma((4,)),
        ],
        compiler_params=pltpu.CompilerParams(
            collective_id=0, has_side_effects=True, vmem_limit_bytes=60 * 2**20
        ),
        name="step",
    )(tokens, gain, weights, ow, rwt, cw, hw, cot)


def finish_kernel(holo_in, own_ref, other_ref, rwt_ref, holo_ref, cg_ref, og_ref):
    col = lax.axis_index("col")
    small = jnp.concatenate([own_ref[320:384, :], own_ref[384:448, :]], axis=1)
    og_ref[...] = dot_nn(jnp.transpose(small.astype(F32)).astype(BF16), rwt_ref[...])
    for at, source in ((col, own_ref), (1 - col, other_ref)):
        for k in range(4):
            cg_ref[at, :, 128 * k : 128 * k + 128] = source[64 * k : 64 * k + 64, :].astype(F32)
        cg_ref[at, :, 512:576] = source[256:320, 0:64].astype(F32)
    holo_ref[0] = holo_in[...]


def finish(holo, own, other, rwt, cw, ow):
    vmem = pl.BlockSpec(memory_space=pltpu.VMEM)
    return pl.pallas_call(
        finish_kernel,
        out_shape=(
            jax.ShapeDtypeStruct((1, *holo.shape), F32),
            jax.ShapeDtypeStruct(cw.shape, F32),
            jax.ShapeDtypeStruct(ow.shape, F32),
        ),
        in_specs=[vmem] * 4,
        out_specs=(vmem,) * 3,
        name="finish",
    )(holo, own, other, rwt)


def shards(
    tokens, ln_gain, qkv_weight, out_weight, readout_weight, conv_weight, head_weight, holo_cot
):
    rows_in = tokens[0]
    rwt = jnp.transpose(readout_weight)
    holo, own, other = step(
        rows_in, ln_gain, qkv_weight, out_weight, rwt, conv_weight, head_weight, holo_cot[0]
    )
    return finish(holo, own, other, rwt, conv_weight, out_weight)


def solution(mesh):
    in_specs = (
        P("dp", "tok", None),
        P(),
        P(None, None, "col"),
        P("col", None),
        P(),
        P(),
        P(),
        P("dp", None, "tok", "col"),
    )
    out_specs = (P("dp", None, "tok", "col"), P(), P("col", None))
    return jax.shard_map(shards, mesh=mesh, in_specs=in_specs, out_specs=out_specs, check_vma=False)
```

```python
import functools

import jax
import jax.numpy as jnp
from jax import lax
from jax.experimental import pallas as pl
from jax.experimental.pallas import tpu as pltpu
from jax.sharding import PartitionSpec as P

HEAD = 64
EPSILON = 1e-05
MESH = pl.DeviceIdType.MESH
F32 = jnp.float32
BF16 = jnp.bfloat16

NT = (((1,), (1,)), ((), ()))


def dot_nt(a, b):
    return lax.dot_general(a, b, NT, preferred_element_type=F32)


def dot_nn(a, b):
    return jnp.dot(a, b, preferred_element_type=F32)


def remote(src, dst, send_sem, recv_sem, where):
    return pltpu.make_async_remote_copy(
        src_ref=src,
        dst_ref=dst,
        send_sem=send_sem,
        recv_sem=recv_sem,
        device_id=where,
        device_id_type=MESH,
    )


QT = 512
LN_ROWS = 128
KT = 512
HALF = 256


def low_lanes(shape):
    return lax.broadcasted_iota(jnp.int32, shape, 1) < HEAD


def swap_lanes(value):
    return pltpu.roll(value.astype(F32), HEAD, 1)


def attention_part(
    ready,
    meanwhile,
    tok_ref,
    gain_ref,
    w_ref,
    ctx_ref,
    normed_ref,
    qout,
    qin,
    qz,
    kvout,
    kvb,
    vx,
    m_ref,
    acc_ref,
    oout,
    oin,
    q_send,
    q_recv,
    d_send,
    m_send,
    c_send,
    kv_recv,
    o_send,
    o_recv,
):
    t = lax.axis_index("tok")
    n_z = lax.axis_size("tok") // 2
    z, c = t // 2, lax.rem(t, 2)
    side = lax.rem(z, 2)
    head = z // 2
    step = 2 * side - 1

    def device(chip, core):
        return {"tok": chip * 2 + core}

    def source(i):
        return device(lax.rem(z + step * i + n_z, n_z), c)

    twin = device(z + 1 - 2 * side, c)
    mate = device(z, 1 - c)

    def target(far):
        way = step * (2 * (far % 2) - 1)
        return lax.rem(z + way * far + 2 * n_z, n_z)

    gain = gain_ref[...].astype(F32).reshape(1, -1)
    low = low_lanes((LN_ROWS, 128))

    def both(r):
        first = pl.ds(pl.multiple_of(r * LN_ROWS, LN_ROWS), LN_ROWS)
        second = pl.ds(pl.multiple_of(HALF + r * LN_ROWS, LN_ROWS), LN_ROWS)
        return first, second

    def project_queries(r, carry):
        first, second = both(r)
        x = jnp.concatenate([tok_ref[first, :], tok_ref[second, :]], axis=0).astype(F32)
        center = x - jnp.mean(x, axis=-1, keepdims=True)
        spread = jnp.mean(center * center, axis=-1, keepdims=True)
        normed = (center * lax.rsqrt(spread + EPSILON) * gain).astype(BF16)
        normed_ref[first, :] = normed[0:LN_ROWS]
        normed_ref[second, :] = normed[LN_ROWS:]
        q = dot_nn(normed, w_ref[0])
        for pair in range(2):
            qt = q[:, 128 * pair : 128 * pair + 128]
            q_top, q_bottom = qt[0:LN_ROWS], qt[LN_ROWS:]
            qout[2 * pair, first, :] = jnp.where(low, q_top, swap_lanes(q_bottom)).astype(BF16)
            qout[2 * pair + 1, first, :] = jnp.where(low, swap_lanes(q_top), q_bottom).astype(BF16)
        return carry

    def project_keys(r, carry):
        first, second = both(r)
        normed = jnp.concatenate([normed_ref[first, :], normed_ref[second, :]], axis=0)
        k = dot_nn(normed, w_ref[1])
        v = dot_nn(normed, w_ref[2])
        for pair in range(2):
            tile = slice(128 * pair, 128 * pair + 128)
            kt, vt = k[:, tile], v[:, tile]
            v_moved, k_moved = swap_lanes(vt), swap_lanes(kt)
            for part, at in ((0, first), (1, second)):
                rows = slice(part * LN_ROWS, (part + 1) * LN_ROWS)
                kvout[2 * pair, at, :] = jnp.where(low, kt[rows], v_moved[rows]).astype(BF16)
                kvout[2 * pair + 1, at, :] = jnp.where(low, k_moved[rows], vt[rows]).astype(BF16)
        return carry

    def send_q(far):
        chip = target(far)
        return remote(
            qout.at[chip // 2], qin.at[far], q_send.at[far], q_recv.at[far], device(chip, c)
        )

    def send_kv(far):
        chip = target(far)
        return remote(
            kvout.at[chip // 2],
            kvb.at[2 * far, c],
            d_send.at[far],
            kv_recv.at[2 * far, c],
            device(chip, c),
        )

    def own(blk):
        return kvout.at[head] if blk == 0 else kvb.at[blk, c]

    def to_twin(i):
        there = 2 * i + 1
        return remote(own(2 * i), kvb.at[there, c], m_send.at[i], kv_recv.at[there, c], twin)

    def to_mate(blk):
        return remote(own(blk), kvb.at[blk, c], c_send.at[blk], kv_recv.at[blk, c], mate)

    def landed(blk, core):
        piece = kvb.at[blk, core]
        remote(piece, piece, c_send.at[blk], kv_recv.at[blk, core], mate).wait_recv()

    lax.fori_loop(0, HALF // LN_ROWS, project_queries, 0)
    ready()
    for far in range(1, 4):
        send_q(far).start()
    lax.fori_loop(0, HALF // LN_ROWS, project_keys, 0)
    to_mate(0).start()
    to_twin(0).start()
    send_kv(1).start()
    kvb[0, c] = kvout[head]
    meanwhile()
    m_ref[...] = jnp.full(m_ref.shape, -1e30, F32)
    acc_ref[...] = jnp.zeros(acc_ref.shape, F32)

    low_h = low_lanes((HALF, 128))

    def unpack(packed):
        value = packed.astype(F32) * (1.0 / HEAD**0.5)
        top = jnp.where(low_h, value, 0.0).astype(BF16)
        bottom = jnp.where(low_h, pltpu.roll(value, HEAD, 1), 0.0).astype(BF16)
        return top, bottom

    def place(i, packed):
        top, bottom = unpack(packed)
        qz[i, 0:HALF, :] = top
        qz[i, HALF : 2 * HALF, :] = bottom

    place(0, qout[head])

    def take(blk, i, at_v):
        for tile in range(2 * HALF // QT):
            at = slice(tile * QT, (tile + 1) * QT)
            q = qz[i, at, :]
            s = [dot_nt(q, kvb[blk, half]) for half in range(2)]
            m_old = m_ref[i, at, :]
            top = jnp.maximum(
                jnp.max(s[0], axis=1, keepdims=True), jnp.max(s[1], axis=1, keepdims=True)
            )
            m_new = jnp.maximum(m_old, top)
            wide = jnp.concatenate([m_new] * (KT // 128), axis=1)
            out = None
            for half in range(2):
                p = jnp.exp(s[half] - wide).astype(BF16)
                o = dot_nn(p, vx[at_v, half])
                out = o if out is None else out + o
            acc_ref[i, at, :] = acc_ref[i, at, :] * jnp.exp(m_old - m_new) + out
            m_ref[i, at, :] = m_new

    def values(blk, at_v):
        low_k = low_lanes((KT, 128))
        for half in range(2):
            v = kvb[blk, half]
            vx[at_v, half] = jnp.where(low_k, jnp.ones_like(v), v)

    def send_o(i):
        return remote(oout.at[i], oin.at[head], o_send.at[i], o_recv.at[head], source(i))

    def relay(blk):
        landed(blk, c)
        remote(
            kvb.at[blk, c],
            kvb.at[blk + 1, c],
            m_send.at[blk // 2],
            kv_recv.at[blk + 1, c],
            twin,
        ).start()
        pass_on(blk)

    def pass_on(blk):
        remote(kvb.at[blk, c], kvb.at[blk, c], c_send.at[blk], kv_recv.at[blk, c], mate).start()

    landed(0, 1 - c)
    values(0, 0)

    def first_block(i, carry):
        @pl.when(i > 0)
        def _():
            remote(qin.at[i], qin.at[i], q_send.at[0], q_recv.at[i], mate).wait_recv()
            top, bottom = unpack(qin[i])
            qz[i, 0:HALF, :] = top
            qz[i, HALF : 2 * HALF, :] = bottom

        take(0, i, 0)

        @pl.when(i == 1)
        def _():
            landed(1, c)
            pass_on(1)

        return carry

    lax.fori_loop(0, 4, first_block, 0)

    def middle(blk, carry):
        @pl.when(blk == 1)
        def _():
            send_kv(2).start()

        @pl.when(blk == 2)
        def _():
            send_kv(3).start()

        landed(blk, 1 - c)
        values(blk, 0)

        def each(i, inner):
            take(blk, i, 0)

            @pl.when(jnp.logical_and(lax.rem(blk, 2) == 1, i == 0))
            def _():
                relay(jnp.minimum(blk + 1, 6))

            @pl.when(jnp.logical_and(lax.rem(blk, 2) == 0, i == 1))
            def _():
                landed(blk + 1, c)
                pass_on(blk + 1)

            return inner

        lax.fori_loop(0, 4, each, 0)
        return carry

    lax.fori_loop(1, 6, middle, 0)

    landed(6, 1 - c)
    values(6, 0)

    def earlier(j, carry):
        take(6, 3 - j, 0)
        return carry

    lax.fori_loop(0, 2, earlier, 0)
    landed(7, c)
    pass_on(7)
    landed(7, 1 - c)
    values(7, 1)

    def last_blocks(j, carry):
        i = 3 - j

        def each(k, inner):
            take(6 + k, i, k)
            return inner

        lax.fori_loop(jnp.where(j < 2, 1, 0), 2, each, 0)
        whole = acc_ref[i]
        done = whole / pltpu.roll(whole, HEAD, 1)
        packed = jnp.where(low_h, pltpu.roll(done[0:HALF], HEAD, 1), done[HALF:])
        oout[i] = packed.astype(BF16)

        @pl.when(i > 0)
        def _():
            send_o(i).start()

        return carry

    lax.fori_loop(0, 4, last_blocks, 0)
    oin[head] = oout[0]

    for k in range(1, 4):
        send_q(k).wait_send()
        send_kv(k).wait_send()
        send_o(k).wait_send()
    for i in range(4):
        to_twin(i).wait_send()
    for blk in range(8):
        to_mate(blk).wait_send()
    for k in range(1, 4):
        h = target(k) // 2
        remote(oin.at[h], oin.at[h], o_send.at[0], o_recv.at[h], mate).wait_recv()

    for pair in range(2):
        even, odd = oin[2 * pair].astype(F32), oin[2 * pair + 1].astype(F32)
        tile = slice(128 * pair, 128 * pair + 128)
        ctx_ref[0:HALF, tile] = jnp.where(low_h, even, pltpu.roll(odd, HEAD, 1)).astype(BF16)
        ctx_ref[HALF : 2 * HALF, tile] = jnp.where(low_h, pltpu.roll(even, HEAD, 1), odd).astype(BF16)


RS_ROWS = 32
CG_TILES = 5
RS_CHUNKS = 14
CG_CHUNKS = 10


def pieces_of(value):
    high = value.astype(BF16)
    rest = value - high.astype(F32)
    mid = rest.astype(BF16)
    low = (rest - mid.astype(F32)).astype(BF16)
    return high, mid, low


def sigmoid(v):
    return 1.0 / (1.0 + jnp.exp(-v))


def step_kernel(
    tok_ref,
    gain_ref,
    w_ref,
    ow_ref,
    rwt_ref,
    cw_ref,
    hw_ref,
    cot_ref,
    holo_ref,
    own_ref,
    other_ref,
    ctx_ref,
    w2_ref,
    base_ref,
    cwt_ref,
    pbuf,
    ext,
    cbuf,
    st1,
    st2,
    sg,
    buf,
    rbuf,
    dbuf,
    fbuf,
    gbuf,
    p_send,
    p_recv,
    h_send,
    h_recv,
    s1,
    r1,
    s2,
    r2,
    s3,
    r3,
    s4,
    r4,
    *attention_refs,
):
    t = lax.axis_index("tok")
    n_t = lax.axis_size("tok")
    dp = lax.axis_index("dp")
    n_dp = lax.axis_size("dp")
    col = lax.axis_index("col")
    other = 1 - col

    barrier = pltpu.get_barrier_semaphore()
    pl.semaphore_signal(barrier, inc=1, device_id={"col": other}, device_id_type=MESH)
    for k in range(1, n_t):
        pl.semaphore_signal(
            barrier, inc=1, device_id={"tok": lax.rem(t + k, n_t)}, device_id_type=MESH
        )
    for k in range(1, n_dp):
        pl.semaphore_signal(
            barrier, inc=1, device_id={"dp": lax.rem(dp + k, n_dp)}, device_id_type=MESH
        )

    to_mate = {"col": other}
    c_copy = remote(cot_ref, cbuf.at[1, col], p_send.at[1], p_recv.at[1], to_mate)

    def ready():
        pl.semaphore_wait(barrier, n_t + n_dp - 1)

    def meanwhile():
        c_copy.start()
        cbuf[1, col] = cot_ref[...]
        for k, piece in enumerate(pieces_of(dot_nt(rwt_ref[...], ow_ref[...]))):
            w2_ref[k] = piece
        base_ref[...] = dot_nt(rwt_ref[...], tok_ref[...])
        for layer in range(2):
            for k in range(9):
                tap = slice(64 * k, 64 * k + 64)
                turned = jnp.transpose(cw_ref[layer, :, tap].astype(F32))
                cwt_ref[layer, :, tap] = turned.astype(BF16)

    attention_part(ready, meanwhile, tok_ref, gain_ref, w_ref, ctx_ref, *attention_refs)

    ctx = ctx_ref[...]
    share = dot_nt(w2_ref[0], ctx) + (dot_nt(w2_ref[1], ctx) + dot_nt(w2_ref[2], ctx))
    pbuf[0] = share.astype(BF16)
    p_copy = remote(pbuf.at[0], pbuf.at[1], p_send.at[0], p_recv.at[0], to_mate)
    p_copy.start()
    p_copy.wait_recv()
    ext[2] = (base_ref[...] + (pbuf[0].astype(F32) + pbuf[1].astype(F32))).astype(BF16)
    c_copy.wait_recv()

    halo = []
    for k, (off, slot) in enumerate(((1, 1), (-1, 3), (2, 0), (-2, 4))):
        peer = {"tok": lax.rem(t + off + n_t, n_t)}
        halo.append(remote(ext.at[2], ext.at[slot], h_send.at[k], h_recv.at[k], peer))
        if k < 2:
            halo.append(
                remote(cbuf.at[1], cbuf.at[2 * k], h_send.at[4 + k], h_recv.at[4 + k], peer)
            )
    for item in halo:
        item.start()
    for item in halo:
        item.wait_recv()

    def in_frame(values, first_row):
        count = values.shape[1]
        row = lax.broadcasted_iota(jnp.int32, (1, count), 1) // 256 + (first_row - 4 + 2 * t)
        inside = jnp.logical_and(row >= 0, row < 2 * n_t)
        return jnp.where(inside, values, 0.0)

    def sides(values):
        count = values.shape[1]
        at = lax.broadcasted_iota(jnp.int32, (1, count), 1) % 256
        before = jnp.where(at == 0, 0.0, pltpu.roll(values, 1, 1))
        after = jnp.where(at == 255, 0.0, pltpu.roll(values, count - 1, 1))
        return before.astype(BF16), values.astype(BF16), after.astype(BF16)

    def stack(target, values, count, flip):
        shifted = sides(values)
        for a in range(3):
            for b in range(3):
                k = (3 * a + b) * 64
                row, piece = (2 - a, shifted[2 - b]) if flip else (a, shifted[b])
                target[k : k + 64, 0:count] = piece[:, row * 256 : row * 256 + count]

    x0 = in_frame(jnp.concatenate([ext[k].astype(F32) for k in range(5)], axis=1), 0)
    stack(st1, x0, 2048, False)
    pre1 = dot_nn(cw_ref[0], st1[...])
    sig1 = sigmoid(pre1)
    h1 = in_frame(pre1 * sig1, 1).astype(BF16)
    stack(st2, h1.astype(F32), 1536, False)
    pre2 = dot_nn(cw_ref[1], st2[...])
    sig2 = sigmoid(pre2)
    own2 = slice(512, 1024)
    h2 = (pre2[:, own2] * sig2[:, own2]).astype(BF16)
    holo = dot_nn(hw_ref[...], h2)
    for row in range(2):
        left = holo[:, row * 256 : row * 256 + 128]
        right = holo[:, row * 256 + 128 : row * 256 + 256]
        holo_ref[:, row, :] = jnp.where(col == 0, left, right)

    diagonal = lax.broadcasted_iota(jnp.int32, (64, 64), 0) == lax.broadcasted_iota(
        jnp.int32, (64, 64), 1
    )
    raised = None
    for k in range(2):
        cot = jnp.concatenate(
            [
                cbuf[s, half, k, row : row + 1, :]
                for s in range(3)
                for row in range(2)
                for half in range(2)
            ],
            axis=1,
        )
        weight = jnp.where(diagonal, hw_ref[k : k + 1, :].astype(F32), 0.0)
        product = jnp.sum(weight, axis=1, keepdims=True) * cot
        raised = product if raised is None else raised + product
    gh2 = raised.astype(BF16)
    gp2 = in_frame(gh2.astype(F32) * sig2 * (1.0 + pre2 * (1.0 - sig2)), 2).astype(BF16)
    stack(sg, gp2.astype(F32), 1024, True)
    gh1 = dot_nn(cwt_ref[1], sg[...]).astype(BF16)
    sig1_in, pre1_in = sig1[:, 512:1536], pre1[:, 512:1536]
    gp1 = in_frame(gh1.astype(F32) * sig1_in * (1.0 + pre1_in * (1.0 - sig1_in)), 3).astype(BF16)
    stack(sg, gp1.astype(F32), 512, True)
    gh0 = dot_nn(cwt_ref[0], sg[:, 0:512]).astype(BF16)

    first = jnp.full((1, 1), col, jnp.int32) == 0
    grad = jnp.where(first, gp1[:, 256:768].astype(F32), gp2[:, own2].astype(F32)).astype(BF16)

    @pl.when(col == 0)
    def _():
        sg[:, 512:1024] = st1[:, 768:1280]

    @pl.when(col == 1)
    def _():
        sg[:, 512:1024] = st2[:, 512:1024]

    term = dot_nt(grad, sg[:, 512:1024])
    for k in range(4):
        buf[64 * k : 64 * k + 64, :] = term[:, 128 * k : 128 * k + 128].astype(BF16)
    buf[256:320, 0:64] = term[:, 512:576].astype(BF16)
    buf[256:320, 64:128] = jnp.zeros((64, 64), BF16)
    small_term = dot_nn(gh0, ctx)
    buf[320:384, :] = small_term[:, 0:128].astype(BF16)
    buf[384:448, :] = small_term[:, 128:256].astype(BF16)

    def chunk(ref, i):
        return ref.at[pl.ds(pl.multiple_of(i * RS_ROWS, RS_ROWS), RS_ROWS), :]

    def phase1(k):
        peer = lax.rem(t + k, n_t)
        return peer, remote(chunk(buf, peer), rbuf.at[t], s1.at[k], r1.at[t], {"tok": peer})

    def arrival1(k):
        source = lax.rem(t + k, n_t)
        return remote(chunk(buf, 0), rbuf.at[source], s1.at[k], r1.at[source], {"tok": source})

    far_first = sorted(range(1, n_t), key=lambda k: -min(k, n_t - k))
    for k in far_first:
        peer, item = phase1(k)

        @pl.when(peer < RS_CHUNKS)
        def _():
            item.start()

    @pl.when(t < RS_CHUNKS)
    def _():
        rbuf[t] = buf[pl.ds(pl.multiple_of(t * RS_ROWS, RS_ROWS), RS_ROWS), :]
        for k in range(1, n_t):
            arrival1(k).wait_recv()
        total = rbuf[0].astype(F32)
        for j in range(1, n_t):
            total = total + rbuf[j].astype(F32)
        dbuf[dp] = total.astype(BF16)
        for k in range(1, n_dp):
            peer = lax.rem(dp + k, n_dp)
            remote(dbuf.at[dp], dbuf.at[dp], s2.at[k], r2.at[dp], {"dp": peer}).start()
        for k in range(1, n_dp):
            source = lax.rem(dp + k, n_dp)
            remote(
                dbuf.at[source], dbuf.at[source], s2.at[k], r2.at[source], {"dp": source}
            ).wait_recv()
        whole = dbuf[0].astype(F32)
        for j in range(1, n_dp):
            whole = whole + dbuf[j].astype(F32)
        fbuf[pl.ds(pl.multiple_of(t * RS_ROWS, RS_ROWS), RS_ROWS), :] = whole.astype(BF16)
        for k in far_first:
            peer = lax.rem(t + k, n_t)
            remote(chunk(fbuf, t), chunk(fbuf, t), s3.at[k], r3.at[t], {"tok": peer}).start()

    def cross(i):
        return remote(chunk(fbuf, i), chunk(gbuf, i), s4.at[i], r4.at[i], to_mate)

    for k in sorted(range(n_t), key=lambda k: min(k, n_t - k)):
        source = lax.rem(t + k, n_t)
        if k > 0:

            @pl.when(source < RS_CHUNKS)
            def _():
                remote(
                    chunk(fbuf, source), chunk(fbuf, source), s3.at[k], r3.at[source], {"tok": source}
                ).wait_recv()

        @pl.when(source < CG_CHUNKS)
        def _():
            cross(source).start()

    own_ref[...] = fbuf[...]
    for i in range(CG_CHUNKS):
        cross(i).wait_recv()
    other_ref[...] = gbuf[...]

    c_copy.wait_send()
    p_copy.wait_send()
    for item in halo:
        item.wait_send()
    for k in range(1, n_t):
        peer, item = phase1(k)

        @pl.when(peer < RS_CHUNKS)
        def _():
            item.wait_send()

    @pl.when(t < RS_CHUNKS)
    def _():
        for k in range(1, n_dp):
            peer = lax.rem(dp + k, n_dp)
            remote(dbuf.at[dp], dbuf.at[dp], s2.at[k], r2.at[dp], {"dp": peer}).wait_send()
        for k in range(1, n_t):
            peer = lax.rem(t + k, n_t)
            remote(chunk(fbuf, t), chunk(fbuf, t), s3.at[k], r3.at[t], {"tok": peer}).wait_send()

    for i in range(CG_CHUNKS):
        cross(i).wait_send()


def step(tokens, gain, weights, ow, rwt, cw, hw, cot):
    rows, width = tokens.shape
    n_tok = lax.axis_size("tok")
    local = weights.shape[2]
    n_t, n_dp = lax.axis_size("tok"), lax.axis_size("dp")
    vmem = pl.BlockSpec(memory_space=pltpu.VMEM)
    dma = pltpu.SemaphoreType.DMA
    return pl.pallas_call(
        step_kernel,
        out_shape=(
            jax.ShapeDtypeStruct(cot.shape, F32),
            jax.ShapeDtypeStruct((448, 128), BF16),
            jax.ShapeDtypeStruct((320, 128), BF16),
        ),
        in_specs=[vmem] * 8,
        out_specs=(vmem,) * 3,
        scratch_shapes=[
            pltpu.VMEM((rows, local), BF16),
            pltpu.VMEM((3, 64, local), BF16),
            pltpu.VMEM((64, rows), F32),
            pltpu.VMEM((2, 64, 576), BF16),
            pltpu.VMEM((2, 64, 512), BF16),
            pltpu.VMEM((5, 64, 512), BF16),
            pltpu.VMEM((3, 2, 2, 2, 128), F32),
            pltpu.VMEM((576, 2048), BF16),
            pltpu.VMEM((576, 1536), BF16),
            pltpu.VMEM((576, 1024), BF16),
            pltpu.VMEM((448, 128), BF16),
            pltpu.VMEM((n_t, RS_ROWS, 128), BF16),
            pltpu.VMEM((n_dp, RS_ROWS, 128), BF16),
            pltpu.VMEM((448, 128), BF16),
            pltpu.VMEM((320, 128), BF16),
            dma((2,)),
            dma((2,)),
            dma((6,)),
            dma((6,)),
            dma((n_t,)),
            dma((n_t,)),
            dma((n_dp,)),
            dma((n_dp,)),
            dma((n_t,)),
            dma((n_t,)),
            dma((CG_CHUNKS,)),
            dma((CG_CHUNKS,)),
            pltpu.VMEM((rows, width), BF16),
            pltpu.VMEM((4, HALF, 128), BF16),
            pltpu.VMEM((4, HALF, 128), BF16),
            pltpu.VMEM((4, rows, 128), BF16),
            pltpu.VMEM((4, rows, 128), BF16),
            pltpu.VMEM((8, 2, rows, 128), BF16),
            pltpu.VMEM((2, 2, rows, 128), BF16),
            pltpu.VMEM((4, rows, 128), F32),
            pltpu.VMEM((4, rows, 128), F32),
            pltpu.VMEM((4, HALF, 128), BF16),
            pltpu.VMEM((4, HALF, 128), BF16),
            dma((4,)),
            dma((4,)),
            dma((4,)),
            dma((4,)),
            dma((8,)),
            dma((8, 2)),
            dma((4,)),
            dma((4,)),
        ],
        compiler_params=pltpu.CompilerParams(
            collective_id=0, has_side_effects=True, vmem_limit_bytes=60 * 2**20
        ),
        name="step",
    )(tokens, gain, weights, ow, rwt, cw, hw, cot)


def finish_kernel(holo_in, own_ref, other_ref, rwt_ref, holo_ref, cg_ref, og_ref):
    col = lax.axis_index("col")
    small = jnp.concatenate([own_ref[320:384, :], own_ref[384:448, :]], axis=1)
    og_ref[...] = dot_nn(jnp.transpose(small.astype(F32)).astype(BF16), rwt_ref[...])
    for at, source in ((col, own_ref), (1 - col, other_ref)):
        for k in range(4):
            cg_ref[at, :, 128 * k : 128 * k + 128] = source[64 * k : 64 * k + 64, :].astype(F32)
        cg_ref[at, :, 512:576] = source[256:320, 0:64].astype(F32)
    holo_ref[0] = holo_in[...]


def finish(holo, own, other, rwt, cw, ow):
    vmem = pl.BlockSpec(memory_space=pltpu.VMEM)
    return pl.pallas_call(
        finish_kernel,
        out_shape=(
            jax.ShapeDtypeStruct((1, *holo.shape), F32),
            jax.ShapeDtypeStruct(cw.shape, F32),
            jax.ShapeDtypeStruct(ow.shape, F32),
        ),
        in_specs=[vmem] * 4,
        out_specs=(vmem,) * 3,
        name="finish",
    )(holo, own, other, rwt)


def shards(
    tokens, ln_gain, qkv_weight, out_weight, readout_weight, conv_weight, head_weight, holo_cot
):
    rows_in = tokens[0]
    rwt = jnp.transpose(readout_weight)
    holo, own, other = step(
        rows_in, ln_gain, qkv_weight, out_weight, rwt, conv_weight, head_weight, holo_cot[0]
    )
    return finish(holo, own, other, rwt, conv_weight, out_weight)


def solution(mesh):
    in_specs = (
        P("dp", "tok", None),
        P(),
        P(None, None, "col"),
        P("col", None),
        P(),
        P(),
        P(),
        P("dp", None, "tok", "col"),
    )
    out_specs = (P("dp", None, "tok", "col"), P(), P("col", None))
    return jax.shard_map(shards, mesh=mesh, in_specs=in_specs, out_specs=out_specs, check_vma=False)
```

```python
import functools

import jax
import jax.numpy as jnp
from jax import lax
from jax.experimental import pallas as pl
from jax.experimental.pallas import tpu as pltpu
from jax.sharding import PartitionSpec as P

HEAD = 64
EPSILON = 1e-05
MESH = pl.DeviceIdType.MESH
F32 = jnp.float32
BF16 = jnp.bfloat16

NT = (((1,), (1,)), ((), ()))


def dot_nt(a, b):
    return lax.dot_general(a, b, NT, preferred_element_type=F32)


def dot_nn(a, b):
    return jnp.dot(a, b, preferred_element_type=F32)


def remote(src, dst, send_sem, recv_sem, where):
    return pltpu.make_async_remote_copy(
        src_ref=src,
        dst_ref=dst,
        send_sem=send_sem,
        recv_sem=recv_sem,
        device_id=where,
        device_id_type=MESH,
    )


QT = 512
LN_ROWS = 128
KT = 512
HALF = 256


def low_lanes(shape):
    return lax.broadcasted_iota(jnp.int32, shape, 1) < HEAD


def swap_lanes(value):
    return pltpu.roll(value.astype(F32), HEAD, 1)


def attention_part(
    ready,
    meanwhile,
    tok_ref,
    gain_ref,
    w_ref,
    ctx_ref,
    normed_ref,
    qout,
    qin,
    qz,
    kvout,
    kvb,
    vx,
    m_ref,
    acc_ref,
    oout,
    oin,
    q_send,
    q_recv,
    d_send,
    m_send,
    c_send,
    kv_recv,
    o_send,
    o_recv,
):
    t = lax.axis_index("tok")
    n_z = lax.axis_size("tok") // 2
    z, c = t // 2, lax.rem(t, 2)
    side = lax.rem(z, 2)
    head = z // 2
    step = 2 * side - 1

    def device(chip, core):
        return {"tok": chip * 2 + core}

    def source(i):
        return device(lax.rem(z + step * i + n_z, n_z), c)

    twin = device(z + 1 - 2 * side, c)
    mate = device(z, 1 - c)

    def target(far):
        way = step * (2 * (far % 2) - 1)
        return lax.rem(z + way * far + 2 * n_z, n_z)

    gain = gain_ref[...].astype(F32).reshape(1, -1)
    low = low_lanes((LN_ROWS, 128))

    def both(r):
        first = pl.ds(pl.multiple_of(r * LN_ROWS, LN_ROWS), LN_ROWS)
        second = pl.ds(pl.multiple_of(HALF + r * LN_ROWS, LN_ROWS), LN_ROWS)
        return first, second

    def project_queries(r, carry):
        first, second = both(r)
        x = jnp.concatenate([tok_ref[first, :], tok_ref[second, :]], axis=0).astype(F32)
        center = x - jnp.mean(x, axis=-1, keepdims=True)
        spread = jnp.mean(center * center, axis=-1, keepdims=True)
        normed = (center * lax.rsqrt(spread + EPSILON) * gain).astype(BF16)
        normed_ref[first, :] = normed[0:LN_ROWS]
        normed_ref[second, :] = normed[LN_ROWS:]
        q = dot_nn(normed, w_ref[0])
        for pair in range(2):
            qt = q[:, 128 * pair : 128 * pair + 128]
            q_top, q_bottom = qt[0:LN_ROWS], qt[LN_ROWS:]
            qout[2 * pair, first, :] = jnp.where(low, q_top, swap_lanes(q_bottom)).astype(BF16)
            qout[2 * pair + 1, first, :] = jnp.where(low, swap_lanes(q_top), q_bottom).astype(BF16)
        return carry

    def project_keys(r, carry):
        first, second = both(r)
        normed = jnp.concatenate([normed_ref[first, :], normed_ref[second, :]], axis=0)
        k = dot_nn(normed, w_ref[1])
        v = dot_nn(normed, w_ref[2])
        for pair in range(2):
            tile = slice(128 * pair, 128 * pair + 128)
            kt, vt = k[:, tile], v[:, tile]
            v_moved, k_moved = swap_lanes(vt), swap_lanes(kt)
            for part, at in ((0, first), (1, second)):
                rows = slice(part * LN_ROWS, (part + 1) * LN_ROWS)
                kvout[2 * pair, at, :] = jnp.where(low, kt[rows], v_moved[rows]).astype(BF16)
                kvout[2 * pair + 1, at, :] = jnp.where(low, k_moved[rows], vt[rows]).astype(BF16)
        return carry

    def send_q(far):
        chip = target(far)
        return remote(
            qout.at[chip // 2], qin.at[far], q_send.at[far], q_recv.at[far], device(chip, c)
        )

    def send_kv(far):
        chip = target(far)
        return remote(
            kvout.at[chip // 2],
            kvb.at[2 * far, c],
            d_send.at[far],
            kv_recv.at[2 * far, c],
            device(chip, c),
        )

    def own(blk):
        return kvout.at[head] if blk == 0 else kvb.at[blk, c]

    def to_twin(i):
        there = 2 * i + 1
        return remote(own(2 * i), kvb.at[there, c], m_send.at[i], kv_recv.at[there, c], twin)

    def to_mate(blk):
        return remote(own(blk), kvb.at[blk, c], c_send.at[blk], kv_recv.at[blk, c], mate)

    def landed(blk, core):
        piece = kvb.at[blk, core]
        remote(piece, piece, c_send.at[blk], kv_recv.at[blk, core], mate).wait_recv()

    lax.fori_loop(0, HALF // LN_ROWS, project_queries, 0)
    ready()
    for far in range(1, 4):
        send_q(far).start()
    lax.fori_loop(0, HALF // LN_ROWS, project_keys, 0)
    to_mate(0).start()
    to_twin(0).start()
    send_kv(1).start()
    kvb[0, c] = kvout[head]
    meanwhile()
    m_ref[...] = jnp.full(m_ref.shape, -1e30, F32)
    acc_ref[...] = jnp.zeros(acc_ref.shape, F32)

    low_h = low_lanes((HALF, 128))

    def unpack(packed):
        value = packed.astype(F32) * (1.0 / HEAD**0.5)
        top = jnp.where(low_h, value, 0.0).astype(BF16)
        bottom = jnp.where(low_h, pltpu.roll(value, HEAD, 1), 0.0).astype(BF16)
        return top, bottom

    def place(i, packed):
        top, bottom = unpack(packed)
        qz[i, 0:HALF, :] = top
        qz[i, HALF : 2 * HALF, :] = bottom

    place(0, qout[head])

    def scores(blk, i):
        return [dot_nt(qz[i], kvb[blk, half]) for half in range(2)]

    def absorb(i, s, at_v):
        m_old = m_ref[i]
        top = jnp.maximum(
            jnp.max(s[0], axis=1, keepdims=True), jnp.max(s[1], axis=1, keepdims=True)
        )
        m_new = jnp.maximum(m_old, top)
        wide = jnp.concatenate([m_new] * (KT // 128), axis=1)
        out = None
        for half in range(2):
            p = jnp.exp(s[half] - wide).astype(BF16)
            o = dot_nn(p, vx[at_v, half])
            out = o if out is None else out + o
        acc_ref[i] = acc_ref[i] * jnp.exp(m_old - m_new) + out
        m_ref[i] = m_new

    def take(blk, i, at_v):
        absorb(i, scores(blk, i), at_v)

    def values(blk, at_v):
        low_k = low_lanes((KT, 128))
        for half in range(2):
            v = kvb[blk, half]
            vx[at_v, half] = jnp.where(low_k, jnp.ones_like(v), v)

    def send_o(i):
        return remote(oout.at[i], oin.at[head], o_send.at[i], o_recv.at[head], source(i))

    def relay(blk):
        landed(blk, c)
        remote(
            kvb.at[blk, c],
            kvb.at[blk + 1, c],
            m_send.at[blk // 2],
            kv_recv.at[blk + 1, c],
            twin,
        ).start()
        pass_on(blk)

    def pass_on(blk):
        remote(kvb.at[blk, c], kvb.at[blk, c], c_send.at[blk], kv_recv.at[blk, c], mate).start()

    landed(0, 1 - c)
    values(0, 0)

    def first_block(i, carry):
        @pl.when(i > 0)
        def _():
            remote(qin.at[i], qin.at[i], q_send.at[0], q_recv.at[i], mate).wait_recv()
            top, bottom = unpack(qin[i])
            qz[i, 0:HALF, :] = top
            qz[i, HALF : 2 * HALF, :] = bottom

        take(0, i, 0)

        @pl.when(i == 1)
        def _():
            landed(1, c)
            pass_on(1)

        return carry

    lax.fori_loop(0, 4, first_block, 0)

    def middle(blk, carry):
        @pl.when(blk == 1)
        def _():
            send_kv(2).start()

        @pl.when(blk == 2)
        def _():
            send_kv(3).start()

        landed(blk, 1 - c)
        values(blk, 0)

        ahead = scores(blk, 0)
        for i in range(4):
            now = ahead
            if i < 3:
                ahead = scores(blk, i + 1)
            absorb(i, now, 0)
            if i == 0:

                @pl.when(lax.rem(blk, 2) == 1)
                def _():
                    relay(jnp.minimum(blk + 1, 6))

            if i == 1:

                @pl.when(lax.rem(blk, 2) == 0)
                def _():
                    landed(blk + 1, c)
                    pass_on(blk + 1)

        return carry

    lax.fori_loop(1, 6, middle, 0)

    landed(6, 1 - c)
    values(6, 0)

    def earlier(j, carry):
        take(6, 3 - j, 0)
        return carry

    lax.fori_loop(0, 2, earlier, 0)
    landed(7, c)
    pass_on(7)
    landed(7, 1 - c)
    values(7, 1)

    def last_blocks(j, carry):
        i = 3 - j

        def each(k, inner):
            take(6 + k, i, k)
            return inner

        lax.fori_loop(jnp.where(j < 2, 1, 0), 2, each, 0)
        whole = acc_ref[i]
        done = whole / pltpu.roll(whole, HEAD, 1)
        packed = jnp.where(low_h, pltpu.roll(done[0:HALF], HEAD, 1), done[HALF:])
        oout[i] = packed.astype(BF16)

        @pl.when(i > 0)
        def _():
            send_o(i).start()

        return carry

    lax.fori_loop(0, 4, last_blocks, 0)
    oin[head] = oout[0]

    for k in range(1, 4):
        send_q(k).wait_send()
        send_kv(k).wait_send()
        send_o(k).wait_send()
    for i in range(4):
        to_twin(i).wait_send()
    for blk in range(8):
        to_mate(blk).wait_send()
    for k in range(1, 4):
        h = target(k) // 2
        remote(oin.at[h], oin.at[h], o_send.at[0], o_recv.at[h], mate).wait_recv()

    for pair in range(2):
        even, odd = oin[2 * pair].astype(F32), oin[2 * pair + 1].astype(F32)
        tile = slice(128 * pair, 128 * pair + 128)
        ctx_ref[0:HALF, tile] = jnp.where(low_h, even, pltpu.roll(odd, HEAD, 1)).astype(BF16)
        ctx_ref[HALF : 2 * HALF, tile] = jnp.where(low_h, pltpu.roll(even, HEAD, 1), odd).astype(BF16)


RS_ROWS = 32
CG_TILES = 5
RS_CHUNKS = 14
CG_CHUNKS = 10


def pieces_of(value):
    high = value.astype(BF16)
    rest = value - high.astype(F32)
    mid = rest.astype(BF16)
    low = (rest - mid.astype(F32)).astype(BF16)
    return high, mid, low


def sigmoid(v):
    return 1.0 / (1.0 + jnp.exp(-v))


def step_kernel(
    tok_ref,
    gain_ref,
    w_ref,
    ow_ref,
    rwt_ref,
    cw_ref,
    hw_ref,
    cot_ref,
    holo_ref,
    own_ref,
    other_ref,
    ctx_ref,
    w2_ref,
    base_ref,
    cwt_ref,
    pbuf,
    ext,
    cbuf,
    st1,
    st2,
    sg,
    buf,
    rbuf,
    dbuf,
    fbuf,
    gbuf,
    p_send,
    p_recv,
    h_send,
    h_recv,
    s1,
    r1,
    s2,
    r2,
    s3,
    r3,
    s4,
    r4,
    *attention_refs,
):
    t = lax.axis_index("tok")
    n_t = lax.axis_size("tok")
    dp = lax.axis_index("dp")
    n_dp = lax.axis_size("dp")
    col = lax.axis_index("col")
    other = 1 - col

    barrier = pltpu.get_barrier_semaphore()
    pl.semaphore_signal(barrier, inc=1, device_id={"col": other}, device_id_type=MESH)
    for k in range(1, n_t):
        pl.semaphore_signal(
            barrier, inc=1, device_id={"tok": lax.rem(t + k, n_t)}, device_id_type=MESH
        )
    for k in range(1, n_dp):
        pl.semaphore_signal(
            barrier, inc=1, device_id={"dp": lax.rem(dp + k, n_dp)}, device_id_type=MESH
        )

    to_mate = {"col": other}
    c_copy = remote(cot_ref, cbuf.at[1, col], p_send.at[1], p_recv.at[1], to_mate)

    def ready():
        pl.semaphore_wait(barrier, n_t + n_dp - 1)

    def meanwhile():
        c_copy.start()
        cbuf[1, col] = cot_ref[...]
        for k, piece in enumerate(pieces_of(dot_nt(rwt_ref[...], ow_ref[...]))):
            w2_ref[k] = piece
        base_ref[...] = dot_nt(rwt_ref[...], tok_ref[...])
        for layer in range(2):
            for k in range(9):
                tap = slice(64 * k, 64 * k + 64)
                turned = jnp.transpose(cw_ref[layer, :, tap].astype(F32))
                cwt_ref[layer, :, tap] = turned.astype(BF16)

    attention_part(ready, meanwhile, tok_ref, gain_ref, w_ref, ctx_ref, *attention_refs)

    ctx = ctx_ref[...]
    share = dot_nt(w2_ref[0], ctx) + (dot_nt(w2_ref[1], ctx) + dot_nt(w2_ref[2], ctx))
    pbuf[0] = share.astype(BF16)
    p_copy = remote(pbuf.at[0], pbuf.at[1], p_send.at[0], p_recv.at[0], to_mate)
    p_copy.start()
    p_copy.wait_recv()
    ext[2] = (base_ref[...] + (pbuf[0].astype(F32) + pbuf[1].astype(F32))).astype(BF16)
    c_copy.wait_recv()

    halo = []
    for k, (off, slot) in enumerate(((1, 1), (-1, 3), (2, 0), (-2, 4))):
        peer = {"tok": lax.rem(t + off + n_t, n_t)}
        halo.append(remote(ext.at[2], ext.at[slot], h_send.at[k], h_recv.at[k], peer))
        if k < 2:
            halo.append(
                remote(cbuf.at[1], cbuf.at[2 * k], h_send.at[4 + k], h_recv.at[4 + k], peer)
            )
    for item in halo:
        item.start()
    for item in halo:
        item.wait_recv()

    def in_frame(values, first_row):
        count = values.shape[1]
        row = lax.broadcasted_iota(jnp.int32, (1, count), 1) // 256 + (first_row - 4 + 2 * t)
        inside = jnp.logical_and(row >= 0, row < 2 * n_t)
        return jnp.where(inside, values, 0.0)

    def sides(values):
        count = values.shape[1]
        at = lax.broadcasted_iota(jnp.int32, (1, count), 1) % 256
        before = jnp.where(at == 0, 0.0, pltpu.roll(values, 1, 1))
        after = jnp.where(at == 255, 0.0, pltpu.roll(values, count - 1, 1))
        return before.astype(BF16), values.astype(BF16), after.astype(BF16)

    def stack(target, values, count, flip):
        shifted = sides(values)
        for a in range(3):
            for b in range(3):
                k = (3 * a + b) * 64
                row, piece = (2 - a, shifted[2 - b]) if flip else (a, shifted[b])
                target[k : k + 64, 0:count] = piece[:, row * 256 : row * 256 + count]

    x0 = in_frame(jnp.concatenate([ext[k].astype(F32) for k in range(5)], axis=1), 0)
    stack(st1, x0, 2048, False)
    pre1 = dot_nn(cw_ref[0], st1[...])
    sig1 = sigmoid(pre1)
    h1 = in_frame(pre1 * sig1, 1).astype(BF16)
    stack(st2, h1.astype(F32), 1536, False)
    pre2 = dot_nn(cw_ref[1], st2[...])
    sig2 = sigmoid(pre2)
    own2 = slice(512, 1024)
    h2 = (pre2[:, own2] * sig2[:, own2]).astype(BF16)
    holo = dot_nn(hw_ref[...], h2)
    for row in range(2):
        left = holo[:, row * 256 : row * 256 + 128]
        right = holo[:, row * 256 + 128 : row * 256 + 256]
        holo_ref[:, row, :] = jnp.where(col == 0, left, right)

    diagonal = lax.broadcasted_iota(jnp.int32, (64, 64), 0) == lax.broadcasted_iota(
        jnp.int32, (64, 64), 1
    )
    raised = None
    for k in range(2):
        cot = jnp.concatenate(
            [
                cbuf[s, half, k, row : row + 1, :]
                for s in range(3)
                for row in range(2)
                for half in range(2)
            ],
            axis=1,
        )
        weight = jnp.where(diagonal, hw_ref[k : k + 1, :].astype(F32), 0.0)
        product = jnp.sum(weight, axis=1, keepdims=True) * cot
        raised = product if raised is None else raised + product
    gh2 = raised.astype(BF16)
    gp2 = in_frame(gh2.astype(F32) * sig2 * (1.0 + pre2 * (1.0 - sig2)), 2).astype(BF16)
    stack(sg, gp2.astype(F32), 1024, True)
    gh1 = dot_nn(cwt_ref[1], sg[...]).astype(BF16)
    sig1_in, pre1_in = sig1[:, 512:1536], pre1[:, 512:1536]
    gp1 = in_frame(gh1.astype(F32) * sig1_in * (1.0 + pre1_in * (1.0 - sig1_in)), 3).astype(BF16)
    stack(sg, gp1.astype(F32), 512, True)
    gh0 = dot_nn(cwt_ref[0], sg[:, 0:512]).astype(BF16)

    first = jnp.full((1, 1), col, jnp.int32) == 0
    grad = jnp.where(first, gp1[:, 256:768].astype(F32), gp2[:, own2].astype(F32)).astype(BF16)

    @pl.when(col == 0)
    def _():
        sg[:, 512:1024] = st1[:, 768:1280]

    @pl.when(col == 1)
    def _():
        sg[:, 512:1024] = st2[:, 512:1024]

    term = dot_nt(grad, sg[:, 512:1024])
    for k in range(4):
        buf[64 * k : 64 * k + 64, :] = term[:, 128 * k : 128 * k + 128].astype(BF16)
    buf[256:320, 0:64] = term[:, 512:576].astype(BF16)
    buf[256:320, 64:128] = jnp.zeros((64, 64), BF16)
    small_term = dot_nn(gh0, ctx)
    buf[320:384, :] = small_term[:, 0:128].astype(BF16)
    buf[384:448, :] = small_term[:, 128:256].astype(BF16)

    def chunk(ref, i):
        return ref.at[pl.ds(pl.multiple_of(i * RS_ROWS, RS_ROWS), RS_ROWS), :]

    def phase1(k):
        peer = lax.rem(t + k, n_t)
        return peer, remote(chunk(buf, peer), rbuf.at[t], s1.at[k], r1.at[t], {"tok": peer})

    def arrival1(k):
        source = lax.rem(t + k, n_t)
        return remote(chunk(buf, 0), rbuf.at[source], s1.at[k], r1.at[source], {"tok": source})

    far_first = sorted(range(1, n_t), key=lambda k: -min(k, n_t - k))
    for k in far_first:
        peer, item = phase1(k)

        @pl.when(peer < RS_CHUNKS)
        def _():
            item.start()

    @pl.when(t < RS_CHUNKS)
    def _():
        rbuf[t] = buf[pl.ds(pl.multiple_of(t * RS_ROWS, RS_ROWS), RS_ROWS), :]
        for k in range(1, n_t):
            arrival1(k).wait_recv()
        total = rbuf[0].astype(F32)
        for j in range(1, n_t):
            total = total + rbuf[j].astype(F32)
        dbuf[dp] = total.astype(BF16)
        for k in range(1, n_dp):
            peer = lax.rem(dp + k, n_dp)
            remote(dbuf.at[dp], dbuf.at[dp], s2.at[k], r2.at[dp], {"dp": peer}).start()
        for k in range(1, n_dp):
            source = lax.rem(dp + k, n_dp)
            remote(
                dbuf.at[source], dbuf.at[source], s2.at[k], r2.at[source], {"dp": source}
            ).wait_recv()
        whole = dbuf[0].astype(F32)
        for j in range(1, n_dp):
            whole = whole + dbuf[j].astype(F32)
        fbuf[pl.ds(pl.multiple_of(t * RS_ROWS, RS_ROWS), RS_ROWS), :] = whole.astype(BF16)
        for k in far_first:
            peer = lax.rem(t + k, n_t)
            remote(chunk(fbuf, t), chunk(fbuf, t), s3.at[k], r3.at[t], {"tok": peer}).start()

    def cross(i):
        return remote(chunk(fbuf, i), chunk(gbuf, i), s4.at[i], r4.at[i], to_mate)

    for k in sorted(range(n_t), key=lambda k: min(k, n_t - k)):
        source = lax.rem(t + k, n_t)
        if k > 0:

            @pl.when(source < RS_CHUNKS)
            def _():
                remote(
                    chunk(fbuf, source), chunk(fbuf, source), s3.at[k], r3.at[source], {"tok": source}
                ).wait_recv()

        @pl.when(source < CG_CHUNKS)
        def _():
            cross(source).start()

    own_ref[...] = fbuf[...]
    for i in range(CG_CHUNKS):
        cross(i).wait_recv()
    other_ref[...] = gbuf[...]

    c_copy.wait_send()
    p_copy.wait_send()
    for item in halo:
        item.wait_send()
    for k in range(1, n_t):
        peer, item = phase1(k)

        @pl.when(peer < RS_CHUNKS)
        def _():
            item.wait_send()

    @pl.when(t < RS_CHUNKS)
    def _():
        for k in range(1, n_dp):
            peer = lax.rem(dp + k, n_dp)
            remote(dbuf.at[dp], dbuf.at[dp], s2.at[k], r2.at[dp], {"dp": peer}).wait_send()
        for k in range(1, n_t):
            peer = lax.rem(t + k, n_t)
            remote(chunk(fbuf, t), chunk(fbuf, t), s3.at[k], r3.at[t], {"tok": peer}).wait_send()

    for i in range(CG_CHUNKS):
        cross(i).wait_send()


def step(tokens, gain, weights, ow, rwt, cw, hw, cot):
    rows, width = tokens.shape
    n_tok = lax.axis_size("tok")
    local = weights.shape[2]
    n_t, n_dp = lax.axis_size("tok"), lax.axis_size("dp")
    vmem = pl.BlockSpec(memory_space=pltpu.VMEM)
    dma = pltpu.SemaphoreType.DMA
    return pl.pallas_call(
        step_kernel,
        out_shape=(
            jax.ShapeDtypeStruct(cot.shape, F32),
            jax.ShapeDtypeStruct((448, 128), BF16),
            jax.ShapeDtypeStruct((320, 128), BF16),
        ),
        in_specs=[vmem] * 8,
        out_specs=(vmem,) * 3,
        scratch_shapes=[
            pltpu.VMEM((rows, local), BF16),
            pltpu.VMEM((3, 64, local), BF16),
            pltpu.VMEM((64, rows), F32),
            pltpu.VMEM((2, 64, 576), BF16),
            pltpu.VMEM((2, 64, 512), BF16),
            pltpu.VMEM((5, 64, 512), BF16),
            pltpu.VMEM((3, 2, 2, 2, 128), F32),
            pltpu.VMEM((576, 2048), BF16),
            pltpu.VMEM((576, 1536), BF16),
            pltpu.VMEM((576, 1024), BF16),
            pltpu.VMEM((448, 128), BF16),
            pltpu.VMEM((n_t, RS_ROWS, 128), BF16),
            pltpu.VMEM((n_dp, RS_ROWS, 128), BF16),
            pltpu.VMEM((448, 128), BF16),
            pltpu.VMEM((320, 128), BF16),
            dma((2,)),
            dma((2,)),
            dma((6,)),
            dma((6,)),
            dma((n_t,)),
            dma((n_t,)),
            dma((n_dp,)),
            dma((n_dp,)),
            dma((n_t,)),
            dma((n_t,)),
            dma((CG_CHUNKS,)),
            dma((CG_CHUNKS,)),
            pltpu.VMEM((rows, width), BF16),
            pltpu.VMEM((4, HALF, 128), BF16),
            pltpu.VMEM((4, HALF, 128), BF16),
            pltpu.VMEM((4, rows, 128), BF16),
            pltpu.VMEM((4, rows, 128), BF16),
            pltpu.VMEM((8, 2, rows, 128), BF16),
            pltpu.VMEM((2, 2, rows, 128), BF16),
            pltpu.VMEM((4, rows, 128), F32),
            pltpu.VMEM((4, rows, 128), F32),
            pltpu.VMEM((4, HALF, 128), BF16),
            pltpu.VMEM((4, HALF, 128), BF16),
            dma((4,)),
            dma((4,)),
            dma((4,)),
            dma((4,)),
            dma((8,)),
            dma((8, 2)),
            dma((4,)),
            dma((4,)),
        ],
        compiler_params=pltpu.CompilerParams(
            collective_id=0, has_side_effects=True, vmem_limit_bytes=60 * 2**20
        ),
        name="step",
    )(tokens, gain, weights, ow, rwt, cw, hw, cot)


def finish_kernel(holo_in, own_ref, other_ref, rwt_ref, holo_ref, cg_ref, og_ref):
    col = lax.axis_index("col")
    small = jnp.concatenate([own_ref[320:384, :], own_ref[384:448, :]], axis=1)
    og_ref[...] = dot_nn(jnp.transpose(small.astype(F32)).astype(BF16), rwt_ref[...])
    for at, source in ((col, own_ref), (1 - col, other_ref)):
        for k in range(4):
            cg_ref[at, :, 128 * k : 128 * k + 128] = source[64 * k : 64 * k + 64, :].astype(F32)
        cg_ref[at, :, 512:576] = source[256:320, 0:64].astype(F32)
    holo_ref[0] = holo_in[...]


def finish(holo, own, other, rwt, cw, ow):
    vmem = pl.BlockSpec(memory_space=pltpu.VMEM)
    return pl.pallas_call(
        finish_kernel,
        out_shape=(
            jax.ShapeDtypeStruct((1, *holo.shape), F32),
            jax.ShapeDtypeStruct(cw.shape, F32),
            jax.ShapeDtypeStruct(ow.shape, F32),
        ),
        in_specs=[vmem] * 4,
        out_specs=(vmem,) * 3,
        name="finish",
    )(holo, own, other, rwt)


def shards(
    tokens, ln_gain, qkv_weight, out_weight, readout_weight, conv_weight, head_weight, holo_cot
):
    rows_in = tokens[0]
    rwt = jnp.transpose(readout_weight)
    holo, own, other = step(
        rows_in, ln_gain, qkv_weight, out_weight, rwt, conv_weight, head_weight, holo_cot[0]
    )
    return finish(holo, own, other, rwt, conv_weight, out_weight)


def solution(mesh):
    in_specs = (
        P("dp", "tok", None),
        P(),
        P(None, None, "col"),
        P("col", None),
        P(),
        P(),
        P(),
        P("dp", None, "tok", "col"),
    )
    out_specs = (P("dp", None, "tok", "col"), P(), P("col", None))
    return jax.shard_map(shards, mesh=mesh, in_specs=in_specs, out_specs=out_specs, check_vma=False)
```

```python
import functools

import jax
import jax.numpy as jnp
from jax import lax
from jax.experimental import pallas as pl
from jax.experimental.pallas import tpu as pltpu
from jax.sharding import PartitionSpec as P

HEAD = 64
EPSILON = 1e-05
MESH = pl.DeviceIdType.MESH
F32 = jnp.float32
BF16 = jnp.bfloat16

NT = (((1,), (1,)), ((), ()))


def dot_nt(a, b):
    return lax.dot_general(a, b, NT, preferred_element_type=F32)


def dot_nn(a, b):
    return jnp.dot(a, b, preferred_element_type=F32)


def remote(src, dst, send_sem, recv_sem, where):
    return pltpu.make_async_remote_copy(
        src_ref=src,
        dst_ref=dst,
        send_sem=send_sem,
        recv_sem=recv_sem,
        device_id=where,
        device_id_type=MESH,
    )


QT = 512
LN_ROWS = 128
KT = 512
HALF = 256


def low_lanes(shape):
    return lax.broadcasted_iota(jnp.int32, shape, 1) < HEAD


def swap_lanes(value):
    return pltpu.roll(value.astype(F32), HEAD, 1)


def attention_part(
    ready,
    meanwhile,
    tok_ref,
    gain_ref,
    w_ref,
    ctx_ref,
    normed_ref,
    qout,
    qin,
    qz,
    kvout,
    kvb,
    vx,
    m_ref,
    acc_ref,
    oout,
    oin,
    q_send,
    q_recv,
    d_send,
    m_send,
    c_send,
    kv_recv,
    o_send,
    o_recv,
):
    t = lax.axis_index("tok")
    n_z = lax.axis_size("tok") // 2
    z, c = t // 2, lax.rem(t, 2)
    side = lax.rem(z, 2)
    head = z // 2
    step = 2 * side - 1

    def device(chip, core):
        return {"tok": chip * 2 + core}

    def source(i):
        return device(lax.rem(z + step * i + n_z, n_z), c)

    twin = device(z + 1 - 2 * side, c)
    mate = device(z, 1 - c)

    def target(far):
        way = step * (2 * (far % 2) - 1)
        return lax.rem(z + way * far + 2 * n_z, n_z)

    gain = gain_ref[...].astype(F32).reshape(1, -1)
    low = low_lanes((LN_ROWS, 128))

    def both(r):
        first = pl.ds(pl.multiple_of(r * LN_ROWS, LN_ROWS), LN_ROWS)
        second = pl.ds(pl.multiple_of(HALF + r * LN_ROWS, LN_ROWS), LN_ROWS)
        return first, second

    def project_queries(r, carry):
        first, second = both(r)
        x = jnp.concatenate([tok_ref[first, :], tok_ref[second, :]], axis=0).astype(F32)
        center = x - jnp.mean(x, axis=-1, keepdims=True)
        spread = jnp.mean(center * center, axis=-1, keepdims=True)
        normed = (center * lax.rsqrt(spread + EPSILON) * gain).astype(BF16)
        normed_ref[first, :] = normed[0:LN_ROWS]
        normed_ref[second, :] = normed[LN_ROWS:]
        q = dot_nn(normed, w_ref[0])
        for pair in range(2):
            qt = q[:, 128 * pair : 128 * pair + 128]
            q_top, q_bottom = qt[0:LN_ROWS], qt[LN_ROWS:]
            qout[2 * pair, first, :] = jnp.where(low, q_top, swap_lanes(q_bottom)).astype(BF16)
            qout[2 * pair + 1, first, :] = jnp.where(low, swap_lanes(q_top), q_bottom).astype(BF16)
        return carry

    def project_keys(r, carry):
        first, second = both(r)
        normed = jnp.concatenate([normed_ref[first, :], normed_ref[second, :]], axis=0)
        k = dot_nn(normed, w_ref[1])
        v = dot_nn(normed, w_ref[2])
        for pair in range(2):
            tile = slice(128 * pair, 128 * pair + 128)
            kt, vt = k[:, tile], v[:, tile]
            v_moved, k_moved = swap_lanes(vt), swap_lanes(kt)
            for part, at in ((0, first), (1, second)):
                rows = slice(part * LN_ROWS, (part + 1) * LN_ROWS)
                kvout[2 * pair, at, :] = jnp.where(low, kt[rows], v_moved[rows]).astype(BF16)
                kvout[2 * pair + 1, at, :] = jnp.where(low, k_moved[rows], vt[rows]).astype(BF16)
        return carry

    def send_q(far):
        chip = target(far)
        return remote(
            qout.at[chip // 2], qin.at[far], q_send.at[far], q_recv.at[far], device(chip, c)
        )

    def send_kv(far):
        chip = target(far)
        return remote(
            kvout.at[chip // 2],
            kvb.at[2 * far, c],
            d_send.at[far],
            kv_recv.at[2 * far, c],
            device(chip, c),
        )

    def own(blk):
        return kvout.at[head] if blk == 0 else kvb.at[blk, c]

    def to_twin(i):
        there = 2 * i + 1
        return remote(own(2 * i), kvb.at[there, c], m_send.at[i], kv_recv.at[there, c], twin)

    def to_mate(blk):
        return remote(own(blk), kvb.at[blk, c], c_send.at[blk], kv_recv.at[blk, c], mate)

    def landed(blk, core):
        piece = kvb.at[blk, core]
        remote(piece, piece, c_send.at[blk], kv_recv.at[blk, core], mate).wait_recv()

    lax.fori_loop(0, HALF // LN_ROWS, project_queries, 0)
    ready()
    for far in range(1, 4):
        send_q(far).start()
    lax.fori_loop(0, HALF // LN_ROWS, project_keys, 0)
    to_mate(0).start()
    to_twin(0).start()
    send_kv(1).start()
    kvb[0, c] = kvout[head]
    meanwhile()
    m_ref[...] = jnp.full(m_ref.shape, -1e30, F32)
    acc_ref[...] = jnp.zeros(acc_ref.shape, F32)

    low_h = low_lanes((HALF, 128))

    def unpack(packed):
        value = packed.astype(F32) * (1.0 / HEAD**0.5)
        top = jnp.where(low_h, value, 0.0).astype(BF16)
        bottom = jnp.where(low_h, pltpu.roll(value, HEAD, 1), 0.0).astype(BF16)
        return top, bottom

    def place(i, packed):
        top, bottom = unpack(packed)
        qz[i, 0:HALF, :] = top
        qz[i, HALF : 2 * HALF, :] = bottom

    place(0, qout[head])

    def scores(blk, i):
        return [dot_nt(qz[i], kvb[blk, half]) for half in range(2)]

    def absorb(i, s, at_v):
        m_old = m_ref[i]
        top = jnp.maximum(
            jnp.max(s[0], axis=1, keepdims=True), jnp.max(s[1], axis=1, keepdims=True)
        )
        m_new = jnp.maximum(m_old, top)
        wide = jnp.concatenate([m_new] * (KT // 128), axis=1)
        out = None
        for half in range(2):
            p = jnp.exp(s[half] - wide).astype(BF16)
            o = dot_nn(p, vx[at_v, half])
            out = o if out is None else out + o
        acc_ref[i] = acc_ref[i] * jnp.exp(m_old - m_new) + out
        m_ref[i] = m_new

    def take(blk, i, at_v):
        absorb(i, scores(blk, i), at_v)

    def values(blk, at_v):
        low_k = low_lanes((KT, 128))
        for half in range(2):
            v = kvb[blk, half]
            vx[at_v, half] = jnp.where(low_k, jnp.ones_like(v), v)

    def send_o(i):
        return remote(oout.at[i], oin.at[head], o_send.at[i], o_recv.at[head], source(i))

    def relay(blk):
        landed(blk, c)
        remote(
            kvb.at[blk, c],
            kvb.at[blk + 1, c],
            m_send.at[blk // 2],
            kv_recv.at[blk + 1, c],
            twin,
        ).start()
        pass_on(blk)

    def pass_on(blk):
        remote(kvb.at[blk, c], kvb.at[blk, c], c_send.at[blk], kv_recv.at[blk, c], mate).start()

    landed(0, 1 - c)
    values(0, 0)

    def first_block(i, carry):
        @pl.when(i > 0)
        def _():
            remote(qin.at[i], qin.at[i], q_send.at[0], q_recv.at[i], mate).wait_recv()
            top, bottom = unpack(qin[i])
            qz[i, 0:HALF, :] = top
            qz[i, HALF : 2 * HALF, :] = bottom

        take(0, i, 0)

        @pl.when(i == 1)
        def _():
            landed(1, c)
            pass_on(1)

        return carry

    lax.fori_loop(0, 4, first_block, 0)

    def middle(blk, carry):
        @pl.when(blk == 1)
        def _():
            send_kv(2).start()

        @pl.when(blk == 2)
        def _():
            send_kv(3).start()

        landed(blk, 1 - c)
        values(blk, 0)

        ahead = scores(blk, 0)
        for i in range(4):
            now = ahead
            if i < 3:
                ahead = scores(blk, i + 1)
            absorb(i, now, 0)
            if i == 0:

                @pl.when(lax.rem(blk, 2) == 1)
                def _():
                    relay(jnp.minimum(blk + 1, 6))

            if i == 1:

                @pl.when(lax.rem(blk, 2) == 0)
                def _():
                    landed(blk + 1, c)
                    pass_on(blk + 1)

        return carry

    lax.fori_loop(1, 6, middle, 0)

    landed(6, 1 - c)
    values(6, 0)

    def earlier(j, carry):
        take(6, 3 - j, 0)
        return carry

    lax.fori_loop(0, 2, earlier, 0)
    landed(7, c)
    pass_on(7)
    landed(7, 1 - c)
    values(7, 1)

    def last_blocks(j, carry):
        i = 3 - j

        def each(k, inner):
            take(6 + k, i, k)
            return inner

        lax.fori_loop(jnp.where(j < 2, 1, 0), 2, each, 0)
        whole = acc_ref[i]
        done = whole / pltpu.roll(whole, HEAD, 1)
        packed = jnp.where(low_h, pltpu.roll(done[0:HALF], HEAD, 1), done[HALF:])
        oout[i] = packed.astype(BF16)

        @pl.when(i > 0)
        def _():
            send_o(i).start()

        return carry

    lax.fori_loop(0, 4, last_blocks, 0)
    oin[head] = oout[0]

    for k in range(1, 4):
        send_q(k).wait_send()
        send_kv(k).wait_send()
        send_o(k).wait_send()
    for i in range(4):
        to_twin(i).wait_send()
    for blk in range(8):
        to_mate(blk).wait_send()
    for k in range(1, 4):
        h = target(k) // 2
        remote(oin.at[h], oin.at[h], o_send.at[0], o_recv.at[h], mate).wait_recv()

    for pair in range(2):
        even, odd = oin[2 * pair].astype(F32), oin[2 * pair + 1].astype(F32)
        tile = slice(128 * pair, 128 * pair + 128)
        ctx_ref[0:HALF, tile] = jnp.where(low_h, even, pltpu.roll(odd, HEAD, 1)).astype(BF16)
        ctx_ref[HALF : 2 * HALF, tile] = jnp.where(low_h, pltpu.roll(even, HEAD, 1), odd).astype(BF16)


RS_ROWS = 32
CG_TILES = 5
RS_CHUNKS = 14
CG_CHUNKS = 10


def pieces_of(value):
    high = value.astype(BF16)
    rest = value - high.astype(F32)
    mid = rest.astype(BF16)
    low = (rest - mid.astype(F32)).astype(BF16)
    return high, mid, low


def sigmoid(v):
    return 1.0 / (1.0 + jnp.exp(-v))


def step_kernel(
    tok_ref,
    gain_ref,
    w_ref,
    ow_ref,
    rwt_ref,
    cw_ref,
    hw_ref,
    cot_ref,
    holo_ref,
    own_ref,
    other_ref,
    ctx_ref,
    w2_ref,
    base_ref,
    cwt_ref,
    pbuf,
    ext,
    cbuf,
    st1,
    st2,
    sg,
    buf,
    rbuf,
    dbuf,
    fbuf,
    gbuf,
    p_send,
    p_recv,
    h_send,
    h_recv,
    s1,
    r1,
    s2,
    r2,
    s3,
    r3,
    s4,
    r4,
    *attention_refs,
):
    t = lax.axis_index("tok")
    n_t = lax.axis_size("tok")
    dp = lax.axis_index("dp")
    n_dp = lax.axis_size("dp")
    col = lax.axis_index("col")
    other = 1 - col

    barrier = pltpu.get_barrier_semaphore()
    pl.semaphore_signal(barrier, inc=1, device_id={"col": other}, device_id_type=MESH)
    for k in range(1, n_t):
        pl.semaphore_signal(
            barrier, inc=1, device_id={"tok": lax.rem(t + k, n_t)}, device_id_type=MESH
        )
    for k in range(1, n_dp):
        pl.semaphore_signal(
            barrier, inc=1, device_id={"dp": lax.rem(dp + k, n_dp)}, device_id_type=MESH
        )

    to_mate = {"col": other}
    c_copy = remote(cot_ref, cbuf.at[1, col], p_send.at[1], p_recv.at[1], to_mate)

    def ready():
        pl.semaphore_wait(barrier, n_t + n_dp - 1)

    def meanwhile():
        c_copy.start()
        cbuf[1, col] = cot_ref[...]
        for k, piece in enumerate(pieces_of(dot_nt(rwt_ref[...], ow_ref[...]))):
            w2_ref[k] = piece
        base_ref[...] = dot_nt(rwt_ref[...], tok_ref[...])
        for layer in range(2):
            for k in range(9):
                tap = slice(64 * k, 64 * k + 64)
                turned = jnp.transpose(cw_ref[layer, :, tap].astype(F32))
                cwt_ref[layer, :, tap] = turned.astype(BF16)

    attention_part(ready, meanwhile, tok_ref, gain_ref, w_ref, ctx_ref, *attention_refs)

    ctx = ctx_ref[...]
    share = dot_nt(w2_ref[0], ctx) + (dot_nt(w2_ref[1], ctx) + dot_nt(w2_ref[2], ctx))
    pbuf[0] = share.astype(BF16)
    p_copy = remote(pbuf.at[0], pbuf.at[1], p_send.at[0], p_recv.at[0], to_mate)
    p_copy.start()
    p_copy.wait_recv()
    ext[2] = (base_ref[...] + (pbuf[0].astype(F32) + pbuf[1].astype(F32))).astype(BF16)
    c_copy.wait_recv()

    halo = []
    for k, (off, slot) in enumerate(((-1, 3), (2, 0), (1, 1), (-2, 4))):
        peer = {"tok": lax.rem(t + off + n_t, n_t)}
        halo.append(remote(ext.at[2], ext.at[slot], h_send.at[k], h_recv.at[k], peer))
        if abs(off) == 1:
            at = 1 - (off + 1) // 2
            halo.append(
                remote(cbuf.at[1], cbuf.at[2 * at], h_send.at[4 + at], h_recv.at[4 + at], peer)
            )
    for item in halo:
        item.start()
    for item in halo:
        item.wait_recv()

    def in_frame(values, first_row):
        count = values.shape[1]
        row = lax.broadcasted_iota(jnp.int32, (1, count), 1) // 256 + (first_row - 4 + 2 * t)
        inside = jnp.logical_and(row >= 0, row < 2 * n_t)
        return jnp.where(inside, values, 0.0)

    def sides(values):
        count = values.shape[1]
        at = lax.broadcasted_iota(jnp.int32, (1, count), 1) % 256
        before = jnp.where(at == 0, 0.0, pltpu.roll(values, 1, 1))
        after = jnp.where(at == 255, 0.0, pltpu.roll(values, count - 1, 1))
        return before.astype(BF16), values.astype(BF16), after.astype(BF16)

    def stack(target, values, count, flip):
        shifted = sides(values)
        for a in range(3):
            for b in range(3):
                k = (3 * a + b) * 64
                row, piece = (2 - a, shifted[2 - b]) if flip else (a, shifted[b])
                target[k : k + 64, 0:count] = piece[:, row * 256 : row * 256 + count]

    x0 = in_frame(jnp.concatenate([ext[k].astype(F32) for k in range(5)], axis=1), 0)
    stack(st1, x0, 2048, False)
    pre1 = dot_nn(cw_ref[0], st1[...])
    sig1 = sigmoid(pre1)
    h1 = in_frame(pre1 * sig1, 1).astype(BF16)
    stack(st2, h1.astype(F32), 1536, False)
    pre2 = dot_nn(cw_ref[1], st2[...])
    sig2 = sigmoid(pre2)
    own2 = slice(512, 1024)
    h2 = (pre2[:, own2] * sig2[:, own2]).astype(BF16)
    holo = dot_nn(hw_ref[...], h2)
    for row in range(2):
        left = holo[:, row * 256 : row * 256 + 128]
        right = holo[:, row * 256 + 128 : row * 256 + 256]
        holo_ref[:, row, :] = jnp.where(col == 0, left, right)

    diagonal = lax.broadcasted_iota(jnp.int32, (64, 64), 0) == lax.broadcasted_iota(
        jnp.int32, (64, 64), 1
    )
    raised = None
    for k in range(2):
        cot = jnp.concatenate(
            [
                cbuf[s, half, k, row : row + 1, :]
                for s in range(3)
                for row in range(2)
                for half in range(2)
            ],
            axis=1,
        )
        weight = jnp.where(diagonal, hw_ref[k : k + 1, :].astype(F32), 0.0)
        product = jnp.sum(weight, axis=1, keepdims=True) * cot
        raised = product if raised is None else raised + product
    gh2 = raised.astype(BF16)
    gp2 = in_frame(gh2.astype(F32) * sig2 * (1.0 + pre2 * (1.0 - sig2)), 2).astype(BF16)
    stack(sg, gp2.astype(F32), 1024, True)
    gh1 = dot_nn(cwt_ref[1], sg[...]).astype(BF16)
    sig1_in, pre1_in = sig1[:, 512:1536], pre1[:, 512:1536]
    gp1 = in_frame(gh1.astype(F32) * sig1_in * (1.0 + pre1_in * (1.0 - sig1_in)), 3).astype(BF16)
    stack(sg, gp1.astype(F32), 512, True)
    gh0 = dot_nn(cwt_ref[0], sg[:, 0:512]).astype(BF16)

    first = jnp.full((1, 1), col, jnp.int32) == 0
    grad = jnp.where(first, gp1[:, 256:768].astype(F32), gp2[:, own2].astype(F32)).astype(BF16)

    @pl.when(col == 0)
    def _():
        sg[:, 512:1024] = st1[:, 768:1280]

    @pl.when(col == 1)
    def _():
        sg[:, 512:1024] = st2[:, 512:1024]

    term = dot_nt(grad, sg[:, 512:1024])
    for k in range(4):
        buf[64 * k : 64 * k + 64, :] = term[:, 128 * k : 128 * k + 128].astype(BF16)
    buf[256:320, 0:64] = term[:, 512:576].astype(BF16)
    buf[256:320, 64:128] = jnp.zeros((64, 64), BF16)
    small_term = dot_nn(gh0, ctx)
    buf[320:384, :] = small_term[:, 0:128].astype(BF16)
    buf[384:448, :] = small_term[:, 128:256].astype(BF16)

    def chunk(ref, i):
        return ref.at[pl.ds(pl.multiple_of(i * RS_ROWS, RS_ROWS), RS_ROWS), :]

    def phase1(k):
        peer = lax.rem(t + k, n_t)
        return peer, remote(chunk(buf, peer), rbuf.at[t], s1.at[k], r1.at[t], {"tok": peer})

    def arrival1(k):
        source = lax.rem(t + k, n_t)
        return remote(chunk(buf, 0), rbuf.at[source], s1.at[k], r1.at[source], {"tok": source})

    far_first = sorted(range(1, n_t), key=lambda k: -min(k, n_t - k))
    for k in far_first:
        peer, item = phase1(k)

        @pl.when(peer < RS_CHUNKS)
        def _():
            item.start()

    @pl.when(t < RS_CHUNKS)
    def _():
        rbuf[t] = buf[pl.ds(pl.multiple_of(t * RS_ROWS, RS_ROWS), RS_ROWS), :]
        for k in range(1, n_t):
            arrival1(k).wait_recv()
        total = rbuf[0].astype(F32)
        for j in range(1, n_t):
            total = total + rbuf[j].astype(F32)
        dbuf[dp] = total.astype(BF16)
        for k in range(1, n_dp):
            peer = lax.rem(dp + k, n_dp)
            remote(dbuf.at[dp], dbuf.at[dp], s2.at[k], r2.at[dp], {"dp": peer}).start()
        for k in range(1, n_dp):
            source = lax.rem(dp + k, n_dp)
            remote(
                dbuf.at[source], dbuf.at[source], s2.at[k], r2.at[source], {"dp": source}
            ).wait_recv()
        whole = dbuf[0].astype(F32)
        for j in range(1, n_dp):
            whole = whole + dbuf[j].astype(F32)
        fbuf[pl.ds(pl.multiple_of(t * RS_ROWS, RS_ROWS), RS_ROWS), :] = whole.astype(BF16)
        for k in far_first:
            peer = lax.rem(t + k, n_t)
            remote(chunk(fbuf, t), chunk(fbuf, t), s3.at[k], r3.at[t], {"tok": peer}).start()

    def cross(i):
        return remote(chunk(fbuf, i), chunk(gbuf, i), s4.at[i], r4.at[i], to_mate)

    for k in sorted(range(n_t), key=lambda k: min(k, n_t - k)):
        source = lax.rem(t + k, n_t)
        if k > 0:

            @pl.when(source < RS_CHUNKS)
            def _():
                remote(
                    chunk(fbuf, source), chunk(fbuf, source), s3.at[k], r3.at[source], {"tok": source}
                ).wait_recv()

        @pl.when(source < CG_CHUNKS)
        def _():
            cross(source).start()

    own_ref[...] = fbuf[...]
    for i in range(CG_CHUNKS):
        cross(i).wait_recv()
    other_ref[...] = gbuf[...]

    c_copy.wait_send()
    p_copy.wait_send()
    for item in halo:
        item.wait_send()
    for k in range(1, n_t):
        peer, item = phase1(k)

        @pl.when(peer < RS_CHUNKS)
        def _():
            item.wait_send()

    @pl.when(t < RS_CHUNKS)
    def _():
        for k in range(1, n_dp):
            peer = lax.rem(dp + k, n_dp)
            remote(dbuf.at[dp], dbuf.at[dp], s2.at[k], r2.at[dp], {"dp": peer}).wait_send()
        for k in range(1, n_t):
            peer = lax.rem(t + k, n_t)
            remote(chunk(fbuf, t), chunk(fbuf, t), s3.at[k], r3.at[t], {"tok": peer}).wait_send()

    for i in range(CG_CHUNKS):
        cross(i).wait_send()


def step(tokens, gain, weights, ow, rwt, cw, hw, cot):
    rows, width = tokens.shape
    n_tok = lax.axis_size("tok")
    local = weights.shape[2]
    n_t, n_dp = lax.axis_size("tok"), lax.axis_size("dp")
    vmem = pl.BlockSpec(memory_space=pltpu.VMEM)
    dma = pltpu.SemaphoreType.DMA
    return pl.pallas_call(
        step_kernel,
        out_shape=(
            jax.ShapeDtypeStruct(cot.shape, F32),
            jax.ShapeDtypeStruct((448, 128), BF16),
            jax.ShapeDtypeStruct((320, 128), BF16),
        ),
        in_specs=[vmem] * 8,
        out_specs=(vmem,) * 3,
        scratch_shapes=[
            pltpu.VMEM((rows, local), BF16),
            pltpu.VMEM((3, 64, local), BF16),
            pltpu.VMEM((64, rows), F32),
            pltpu.VMEM((2, 64, 576), BF16),
            pltpu.VMEM((2, 64, 512), BF16),
            pltpu.VMEM((5, 64, 512), BF16),
            pltpu.VMEM((3, 2, 2, 2, 128), F32),
            pltpu.VMEM((576, 2048), BF16),
            pltpu.VMEM((576, 1536), BF16),
            pltpu.VMEM((576, 1024), BF16),
            pltpu.VMEM((448, 128), BF16),
            pltpu.VMEM((n_t, RS_ROWS, 128), BF16),
            pltpu.VMEM((n_dp, RS_ROWS, 128), BF16),
            pltpu.VMEM((448, 128), BF16),
            pltpu.VMEM((320, 128), BF16),
            dma((2,)),
            dma((2,)),
            dma((6,)),
            dma((6,)),
            dma((n_t,)),
            dma((n_t,)),
            dma((n_dp,)),
            dma((n_dp,)),
            dma((n_t,)),
            dma((n_t,)),
            dma((CG_CHUNKS,)),
            dma((CG_CHUNKS,)),
            pltpu.VMEM((rows, width), BF16),
            pltpu.VMEM((4, HALF, 128), BF16),
            pltpu.VMEM((4, HALF, 128), BF16),
            pltpu.VMEM((4, rows, 128), BF16),
            pltpu.VMEM((4, rows, 128), BF16),
            pltpu.VMEM((8, 2, rows, 128), BF16),
            pltpu.VMEM((2, 2, rows, 128), BF16),
            pltpu.VMEM((4, rows, 128), F32),
            pltpu.VMEM((4, rows, 128), F32),
            pltpu.VMEM((4, HALF, 128), BF16),
            pltpu.VMEM((4, HALF, 128), BF16),
            dma((4,)),
            dma((4,)),
            dma((4,)),
            dma((4,)),
            dma((8,)),
            dma((8, 2)),
            dma((4,)),
            dma((4,)),
        ],
        compiler_params=pltpu.CompilerParams(
            collective_id=0, has_side_effects=True, vmem_limit_bytes=60 * 2**20
        ),
        name="step",
    )(tokens, gain, weights, ow, rwt, cw, hw, cot)


def finish_kernel(holo_in, own_ref, other_ref, rwt_ref, holo_ref, cg_ref, og_ref):
    col = lax.axis_index("col")
    small = jnp.concatenate([own_ref[320:384, :], own_ref[384:448, :]], axis=1)
    og_ref[...] = dot_nn(jnp.transpose(small.astype(F32)).astype(BF16), rwt_ref[...])
    for at, source in ((col, own_ref), (1 - col, other_ref)):
        for k in range(4):
            cg_ref[at, :, 128 * k : 128 * k + 128] = source[64 * k : 64 * k + 64, :].astype(F32)
        cg_ref[at, :, 512:576] = source[256:320, 0:64].astype(F32)
    holo_ref[0] = holo_in[...]


def finish(holo, own, other, rwt, cw, ow):
    vmem = pl.BlockSpec(memory_space=pltpu.VMEM)
    return pl.pallas_call(
        finish_kernel,
        out_shape=(
            jax.ShapeDtypeStruct((1, *holo.shape), F32),
            jax.ShapeDtypeStruct(cw.shape, F32),
            jax.ShapeDtypeStruct(ow.shape, F32),
        ),
        in_specs=[vmem] * 4,
        out_specs=(vmem,) * 3,
        name="finish",
    )(holo, own, other, rwt)


def shards(
    tokens, ln_gain, qkv_weight, out_weight, readout_weight, conv_weight, head_weight, holo_cot
):
    rows_in = tokens[0]
    rwt = jnp.transpose(readout_weight)
    holo, own, other = step(
        rows_in, ln_gain, qkv_weight, out_weight, rwt, conv_weight, head_weight, holo_cot[0]
    )
    return finish(holo, own, other, rwt, conv_weight, out_weight)


def solution(mesh):
    in_specs = (
        P("dp", "tok", None),
        P(),
        P(None, None, "col"),
        P("col", None),
        P(),
        P(),
        P(),
        P("dp", None, "tok", "col"),
    )
    out_specs = (P("dp", None, "tok", "col"), P(), P("col", None))
    return jax.shard_map(shards, mesh=mesh, in_specs=in_specs, out_specs=out_specs, check_vma=False)
```
